256 devices in a mesh: azim: 128 (over x_hi, y, z, core), rad: 2 (over x_lo).
Axes of the slice: x: 4 (x_hi: 2, x_lo: 2; x = x_hi * 2 + x_lo), y: 4, z: 8, core: 2. Of those that a mesh axis runs over, the one named last changes fastest.
Arguments:
- acoustic_state: float32 [5, 1024, 32, 128], P(None, 'azim', 'rad'), may hold values from -6 to 6
- mean_flow: float32 [3, 32, 128], P(None, 'rad'), may hold values from -0.5 to 0.5
- sector_offset: int32 [2], replicated, may hold values from 0 to 127
- cell_shift: int32 [2, 1024], P(None, 'azim'), may hold values from -3 to 0
- stencil_start: int32 [2, 1024], P(None, 'azim'), may hold values from 0 to 1
- interface_fraction: float32 [2, 1024], P(None, 'azim'), may hold values from 0 to 1
Outputs:
- next_state: float32 [5, 1024, 32, 128], P(None, 'azim', 'rad')
The draws below stay inside these ranges and needn't reach their ends.
All inputs are finite; a program needn't handle non-finite values.
Results may differ from the reference program's by a relative error of at most 0.00005.
Values sent between devices are 32-bit elements; how exact they have to be, the bound alone decides.
A program may use at most 64 MiB of HBM per device.

```python
import jax
import jax.numpy as jnp
from jax import lax

CA = 8
CX = 128
STEPS = 2
NA = 1024
NR = 32
N_AZIM = 128


def plant(values, stream_key, least, top_value):
    longest = values.shape.index(max(values.shape))
    spots = []
    for shift in (0, 1):
        where = [jax.random.randint(jax.random.fold_in(stream_key, axis), (), 0, length) for axis, length in enumerate(values.shape)]
        where[longest] = (where[longest] + shift) % values.shape[longest]
        spots.append(tuple(where))
    return values.at[spots[0]].set(least).at[spots[1]].set(top_value)


def levels(own_key, extent, split, smallest, largest):
    def one(axis_at, parts):
        heights = jax.random.uniform(jax.random.fold_in(jax.random.fold_in(own_key, 6), axis_at), (parts,), jnp.float32, smallest / len(split), largest / len(split))
        return jnp.repeat(jnp.exp(heights), extent[axis_at] // parts).reshape((-1,) + (1,) * (len(extent) - axis_at - 1))

    level = one(*split[0])
    for cut in split[1:]:
        level = level * one(*cut)
    return level


def noise(own_key, extent, width, most, cuts=(), kind=jnp.bfloat16):
    entries = jax.random.normal(own_key, extent, jnp.float32) * width
    if len(cuts) > 0:
        entries = levels(own_key, extent, cuts, -0.22, 0.18) * entries
    return jnp.clip(entries, min=-most, max=most).astype(kind)


def setup_inputs(seed: int = 0) -> dict:
    streams_of = jax.random.split(jax.random.key(seed), 7)
    acoustic_state = noise(streams_of[0], (5, NA, NR, CX), 1.0, 6.0, ((1, 128), (2, 2)), jnp.float32)
    mean_flow = jnp.clip(jax.random.uniform(streams_of[1], (3, NR, CX), jnp.float32, -0.5, 0.5) * levels(streams_of[1], (3, NR, CX), ((1, 2),), -0.4, 0.0), -0.5, 0.5)
    sector_offset = jax.random.randint(streams_of[2], (STEPS,), 0, N_AZIM).astype(jnp.int32)
    cell_shift = plant(jax.random.randint(streams_of[3], (STEPS, NA), -3, 1), jax.random.fold_in(streams_of[3], 1), -3, 0).astype(jnp.int32)
    stencil_start = plant(jax.random.randint(streams_of[4], (2, NA), 0, 2), jax.random.fold_in(streams_of[4], 1), 0, 1).astype(jnp.int32)
    interface_fraction = jnp.clip(1.0 * jax.random.uniform(streams_of[5], (2, NA), jnp.float32) ** levels(streams_of[5], (2, NA), ((1, 128),), -0.2, 0.2), 0.0, 1.0)
    return dict(acoustic_state=acoustic_state, mean_flow=mean_flow, sector_offset=sector_offset, cell_shift=cell_shift, stencil_start=stencil_start, interface_fraction=interface_fraction)


STENCIL = (0.841570125482, -0.244678631765, 0.059463584768, -0.007650904064)
STEP_SIZE = 0.2


def derive(extended, along_dim, length):
    summed = None
    for shift_no in range(4):
        forward = lax.slice_in_dim(extended, 5 + shift_no, 5 + shift_no + length, axis=along_dim)
        behind = lax.slice_in_dim(extended, 3 - shift_no, 3 - shift_no + length, axis=along_dim)
        addend = STENCIL[shift_no] * (forward - behind)
        summed = addend if summed is None else summed + addend
    return summed


def lagrange(fraction):
    up_one = fraction + 1.0
    down_one = fraction - 1.0
    down_two = fraction - 2.0
    return jnp.stack([-fraction * down_one * down_two / 6.0, up_one * down_one * down_two / 2.0,
                      -up_one * fraction * down_two / 2.0, up_one * fraction * down_one / 6.0], axis=-1)


def blend(rim_block, first_cell, weights, total_cells):
    summed = jnp.zeros(rim_block.shape, jnp.float32)
    for point_no in range(4):
        source = jnp.mod(first_cell + point_no, total_cells).astype(jnp.int32)
        summed = summed + weights[:, point_no][None, :, None, None] * jnp.take(rim_block, source, axis=1)
    return summed


def evaluate(current, mean_flow, offset, cell_move, stencil_start, interface_fraction):
    total_cells = current.shape[1]
    radial = current.shape[2]
    axial_cells = current.shape[3]
    middle = axial_cells // 2
    beside_all = jnp.concatenate([current[:, -4:], current, current[:, :4]], axis=1)
    beside = jnp.pad(current, ((0, 0), (0, 0), (4, 4), (0, 0)))
    index_cells = jnp.arange(total_cells, dtype=jnp.int32)
    stator_first = index_cells - offset * CA + cell_move + stencil_start[0] - 1
    rotor_first = index_cells + offset * CA - cell_move + stencil_start[1] - 4
    stator_ghost = blend(current[:, :, :, middle:middle + 4], stator_first, lagrange(interface_fraction[0]), total_cells)
    rotor_ghost = blend(current[:, :, :, middle - 4:middle], rotor_first, lagrange(interface_fraction[1]), total_cells)
    zero_pad = jnp.zeros(current.shape[:3] + (4,), jnp.float32)
    stator_line = jnp.concatenate([zero_pad, current[:, :, :, :middle], stator_ghost], axis=3)
    rotor_line = jnp.concatenate([rotor_ghost, current[:, :, :, middle:], zero_pad], axis=3)
    axial_slope = jnp.concatenate([derive(stator_line, 3, middle), derive(rotor_line, 3, axial_cells - middle)], axis=3)
    azim_slope = derive(beside_all, 1, total_cells)
    radial_slope = derive(beside, 2, radial)
    flow_axial = mean_flow[0][None, None]
    flow_radial = mean_flow[1][None, None]
    flow_azim = mean_flow[2][None, None]
    advect = flow_axial * axial_slope + flow_radial * radial_slope + flow_azim * azim_slope
    spread = axial_slope[1] + radial_slope[2] + azim_slope[3]
    forcing = jnp.stack([spread, axial_slope[4], radial_slope[4], azim_slope[4], spread])
    return -advect - forcing


def reference(acoustic_state, mean_flow, sector_offset, cell_shift, stencil_start, interface_fraction):
    current = acoustic_state
    for step_no in range(STEPS):
        offset = sector_offset[step_no]
        cell_move = cell_shift[step_no]
        midpoint = current + (0.5 * STEP_SIZE) * evaluate(current, mean_flow, offset, cell_move, stencil_start, interface_fraction)
        current = current + STEP_SIZE * evaluate(midpoint, mean_flow, offset, cell_move, stencil_start, interface_fraction)
    return current
```

```python
import jax
import jax.numpy as jnp
from jax import lax
from jax.experimental import pallas as pl
from jax.experimental.pallas import tpu as pltpu
from jax.sharding import PartitionSpec as P

STENCIL = (0.841570125482, -0.244678631765, 0.059463584768, -0.007650904064)
STEP_SIZE = 0.2
MESH = pl.DeviceIdType.MESH
F32 = jnp.float32

NZ, NY, NX = 8, 4, 2
N = 128


def lanes(rows=8):
    return lax.broadcasted_iota(jnp.int32, (rows, 128), 1)


def moved(value, by):
    return value if by % 128 == 0 else pltpu.roll(value, (-by) % 128, value.ndim - 1)


def forcing(dx, dr, da):
    spread = dx[1] + dr[2] + da[3]
    return [spread, dx[4], dr[4], da[4], spread]


def kernel(offset_ref, shift_ref, start_ref, fraction_ref, flow_hbm, state_hbm, out_hbm,
           E, mid, slot_c0, slot_c1, slot_z0, slot_z1, slot_y0, slot_y1, slot_x0, slot_x1, facing, own_coef, flow, flow_pack,
           own_pack, face_pad, slope, face_mid, own_fix, fix_wide,
           send_sem, recv_sem, fixed_send, fixed_recv, local_sem):
    slots_c, slots_z, slots_y, slots_x = (slot_c0, slot_c1), (slot_z0, slot_z1), (slot_y0, slot_y1), (slot_x0, slot_x1)
    i = lax.axis_index("azim")
    r = lax.axis_index("rad")
    core, z, y, x = i % 2, (i // 2) % NZ, (i // 16) % NY, i // 64
    row0 = pl.multiple_of(8 + 8 * r, 8)
    far0 = pl.multiple_of(8 + 16 * r, 8)
    up, down = (i + 1) % N, (i + N - 1) % N

    def at(azim, rad=None):
        return {"azim": azim, "rad": r if rad is None else rad}

    core_to = i + 1 - 2 * core
    z_to = [i - 2 * z + 2 * ((z + d) % NZ) for d in range(1, NZ)]
    y_to = [i - 16 * y + 16 * ((y + d) % NY) for d in range(1, NY)]
    x_to = (i + 64) % N

    load = pltpu.make_async_copy(state_hbm, E.at[0, :, pl.ds(8, 8), pl.ds(row0, 16), :], local_sem.at[0])
    load.start()
    load_flow = pltpu.make_async_copy(flow_hbm, flow.at[:, pl.ds(pl.multiple_of(8 * r, 8), 16), :], local_sem.at[1])
    load_flow.start()

    barrier = pltpu.get_barrier_semaphore()
    partners = [at(core_to)] + [at(j) for j in z_to] + [at(j) for j in y_to] + [at(x_to)]
    partners += [at(up), at(down), at(i, 1 - r), at(up, 1 - r), at(down, 1 - r)]
    for partner in partners:
        pl.semaphore_signal(barrier, inc=1, device_id=partner, device_id_type=MESH)

    edge = jnp.zeros((5, 16, 8, 128), F32)
    corner = jnp.zeros((5, 4, 8, 128), F32)
    for n in range(2):
        E[n, :, 4:20, 0:8, :] = edge
        E[n, :, 4:20, 32:40, :] = edge
        far_own = pl.multiple_of(24 - 16 * r, 8)
        E[n, :, 0:4, pl.ds(far_own, 8), :] = corner
        E[n, :, 20:24, pl.ds(far_own, 8), :] = corner
    mid[:, :, 0:8, :] = edge
    mid[:, :, 32:40, :] = edge
    face_pad[:, :, 0:8, :] = jnp.zeros((5, 3, 8, 128), F32)
    face_pad[:, :, 32:40, :] = jnp.zeros((5, 3, 8, 128), F32)

    lane = lanes()
    cell_of = lane // 16
    upper = lane % 16 >= 8
    row = lax.broadcasted_iota(jnp.int32, (8, 128), 0)

    def spread_cells(get):
        value = jnp.full((8, 128), get(0))
        for a in range(1, 8):
            value = jnp.where(cell_of == a, get(a), value)
        return value

    def weights(t, m):
        up_one, down_one, down_two = t + 1.0, t - 1.0, t - 2.0
        w = (-t * down_one * down_two / 6.0, up_one * down_one * down_two / 2.0,
             -up_one * t * down_two / 2.0, up_one * t * down_one / 6.0)
        value = jnp.zeros((8, 128), F32)
        for p in range(4):
            value = jnp.where(m == p, w[p], value)
        return value

    stator_t = spread_cells(lambda a: fraction_ref[0, a])
    rotor_t = spread_cells(lambda a: fraction_ref[1, a])
    for n in range(2):
        stator = weights(stator_t, row - spread_cells(lambda a: shift_ref[n, a] + start_ref[0, a] + 3))
        rotor = weights(rotor_t, row - spread_cells(lambda a: start_ref[1, a] - shift_ref[n, a]))
        own_coef[1, n] = jnp.where(upper, stator, rotor)
        slots_c[n][core, 10] = jnp.where(upper, rotor, stator)

    load.wait()
    load_flow.wait()
    pl.semaphore_wait(barrier, len(partners))

    fixed = []

    def send_fixed(src, dst, to):
        no = len(fixed)
        copy = pltpu.make_async_remote_copy(src, dst, fixed_send.at[no], fixed_recv.at[no], device_id=to, device_id_type=MESH)
        copy.start()
        fixed.append(copy)

    send_fixed(own_coef.at[1], own_coef.at[0], at(up))
    send_fixed(own_coef.at[1], own_coef.at[2], at(down))
    send_fixed(flow.at[:, pl.ds(8, 8), :], flow.at[:, pl.ds(pl.multiple_of(16 * r, 8), 8), :], at(i, 1 - r))

    half = lane % 64
    strip = lane % 16
    ahead = [jnp.where(half + j < 64, STENCIL[j - 1], 0.0) for j in range(1, 5)]
    behind = [jnp.where(half - j >= 0, STENCIL[j - 1], 0.0) for j in range(1, 5)]

    def tall(v):
        return jnp.concatenate([v, v, v], axis=0)

    in_ahead = [tall(jnp.where(strip % 8 + j < 8, STENCIL[j - 1], 0.0)) for j in range(1, 5)]
    in_behind = [tall(jnp.where(strip % 8 - j >= 0, STENCIL[j - 1], 0.0)) for j in range(1, 5)]
    cross_ahead = [tall(jnp.where((strip < 8) & (strip + j >= 8), STENCIL[j - 1], 0.0)) for j in range(1, 5)]
    cross_behind = [tall(jnp.where((strip >= 8) & (strip - j < 8), STENCIL[j - 1], 0.0)) for j in range(1, 5)]
    lane24 = lanes(24)

    def taps(value, fore, aft):
        total = None
        for j in range(1, 5):
            term = fore[j - 1] * moved(value, j) - aft[j - 1] * moved(value, -j)
            total = term if total is None else total + term
        return total

    def by_cells(packs, d, outs=(0, 1, 2)):
        if d == 0:
            return [packs[p] for p in outs]
        turned = [moved(v, 16 * d) for v in packs]
        given = []
        for p in outs:
            q = p + (1 if d > 0 else -1)
            if q < 0 or q > 2:
                given.append(turned[p])
            elif d > 0:
                given.append(jnp.where(lane24 < 128 - 16 * d, turned[p], turned[q]))
            else:
                given.append(jnp.where(lane24 >= -16 * d, turned[p], turned[q]))
        return given

    def evaluate_rows(ref, c, t):
        low = 8 + 8 * t
        dx, dr, da, mine = [], [], [], []
        for f in range(5):
            here = ref[f, c, low:low + 8, :]
            mine.append(here)
            dx.append(taps(here, ahead, behind))
            radial = azimuthal = None
            for j in range(1, 5):
                step = STENCIL[j - 1] * (ref[f, c, low + j:low + j + 8, :] - ref[f, c, low - j:low - j + 8, :])
                radial = step if radial is None else radial + step
                step = STENCIL[j - 1] * (ref[f, c + j, low:low + 8, :] - ref[f, c - j, low:low + 8, :])
                azimuthal = step if azimuthal is None else azimuthal + step
            dr.append(radial)
            da.append(azimuthal)
        u = [flow[k, 8 * t:8 * t + 8, :] for k in range(3)]
        push = forcing(dx, dr, da)
        return mine, [-(u[0] * dx[f] + u[1] * dr[f] + u[2] * da[f]) - push[f] for f in range(5)]

    def pack_own(n, t):
        for f in range(5):
            rows = pl.ds(pl.multiple_of(row0 + 8 * t, 8), 8)
            packed = None
            for a in range(8):
                turned = moved(E[n, f, 8 + a, rows, :], 56 - 16 * a)
                packed = turned if packed is None else jnp.where(cell_of == a, turned, packed)
            slots_c[n][core, t * 5 + f] = packed

    def step(n):
        slot_c, slot_z, slot_y, slot_x = slots_c[n], slots_z[n], slots_y[n], slots_x[n]
        k = offset_ref[n]
        source_r = (i - k + N) % N
        source_s = (i + k) % N
        number = [0]
        started = []

        def send(src, dst, to):
            no = number[0]
            number[0] += 1
            copy = pltpu.make_async_remote_copy(src, dst, send_sem.at[n, no], recv_sem.at[n, no], device_id=to, device_id_type=MESH)
            copy.start()
            started.append(copy)
            return copy

        def chosen(slots, digit):
            from_r, from_s = digit(source_r), digit(source_s)
            return jnp.where(upper[None], slots[from_r], slots[from_s])

        pack_own(n, 0)
        pack_own(n, 1)
        mine = slot_c.at[core]
        stage = [send(mine, mine, at(core_to))]
        for copy in stage:
            copy.wait_recv()

        slot_z[z] = chosen(slot_c, lambda s: s % 2)
        mine = slot_z.at[z]
        stage = [send(mine, mine, at(j)) for j in z_to]
        halos = []
        own_rows, far_rows = pl.ds(row0, 16), pl.ds(far0, 8)
        halos.append(send(E.at[n, :, pl.ds(8, 8), own_rows, :], E.at[n, :, pl.ds(0, 8), own_rows, :], at(up)))
        halos.append(send(E.at[n, :, pl.ds(8, 8), own_rows, :], E.at[n, :, pl.ds(16, 8), own_rows, :], at(down)))
        halos.append(send(E.at[n, :, pl.ds(8, 8), pl.ds(16, 8), :], E.at[n, :, pl.ds(8, 8), far_rows, :], at(i, 1 - r)))
        halos.append(send(E.at[n, :, pl.ds(12, 4), pl.ds(16, 8), :], E.at[n, :, pl.ds(4, 4), far_rows, :], at(up, 1 - r)))
        halos.append(send(E.at[n, :, pl.ds(8, 4), pl.ds(16, 8), :], E.at[n, :, pl.ds(16, 4), far_rows, :], at(down, 1 - r)))
        for copy in stage:
            copy.wait_recv()

        slot_y[y] = chosen(slot_z, lambda s: (s // 2) % NZ)
        mine = slot_y.at[y]
        stage = [send(mine, mine, at(j)) for j in y_to]
        for copy in stage:
            copy.wait_recv()

        slot_x[x] = chosen(slot_y, lambda s: (s // 16) % NY)
        mine = slot_x.at[x]
        stage = [send(mine, mine, at(x_to))]
        for copy in halos:
            copy.wait_recv()

        def first(c, carry):
            for t in range(3):
                here, slopes = evaluate_rows(E.at[n], c + 4, t)
                for f in range(5):
                    mid[f, c, 8 + 8 * t:16 + 8 * t, :] = here[f] + (0.5 * STEP_SIZE) * slopes[f]
            return carry

        lax.fori_loop(0, 16, first, 0)

        def strip_of(f, carry):
            for p in range(3):
                packed = None
                for a in range(8):
                    turned = moved(E[n, f, 8 * p + a, 8:32, :], 56 - 16 * a)
                    packed = turned if packed is None else jnp.where(lane24 // 16 == a, turned, packed)
                own_pack[f, p] = packed
            return carry

        lax.fori_loop(0, 5, strip_of, 0)
        for copy in stage:
            copy.wait_recv()

        got = chosen(slot_x, lambda s: s // 64)
        facing[n, 1, pl.ds(5 * r, 10)] = got[0:10]
        facing[n, 1, 15] = got[10]
        rows10, rows5 = pl.ds(5 * r, 10), pl.ds(10 * r, 5)
        stage = []
        for to, place in ((up, 0), (down, 2)):
            stage.append(send(facing.at[n, 1, rows10], facing.at[n, place, rows10], at(to)))
            stage.append(send(facing.at[n, 1, 15], facing.at[n, place, 15], at(to)))
            stage.append(send(facing.at[n, 1, pl.ds(5, 5)], facing.at[n, place, rows5], at(to, 1 - r)))
        stage.append(send(facing.at[n, 1, pl.ds(5, 5)], facing.at[n, 1, rows5], at(i, 1 - r)))
        for copy in stage:
            copy.wait_recv()

        coef_own = [own_coef[p, n] for p in range(3)]
        coef_face = []
        for p in range(3):
            sent = facing[n, p, 15]
            coef_face.append(jnp.where(upper, moved(sent, -8), moved(sent, 8)))

        def strip_slopes(f, carry):
            F = [jnp.concatenate([facing[n, p, 5 * t + f] for t in range(3)], axis=0) for p in range(3)]
            M = [own_pack[f, p] for p in range(3)]
            for p in range(3):
                face_pad[f, p, 8:32, :] = F[p]
            ghost_own = [jnp.zeros((24, 128), F32)] * 3
            ghost_face = [jnp.zeros((24, 128), F32)] * 3
            azimuthal = [jnp.zeros((24, 128), F32)] * 3
            for d in range(-4, 5):
                shifted = by_cells(F, d)
                if d < 4:
                    shifted_own = by_cells(M, d)
                for p in range(3):
                    if d != 0:
                        weight = STENCIL[d - 1] if d > 0 else -STENCIL[-d - 1]
                        azimuthal[p] = azimuthal[p] + weight * shifted[p]
                    if d < 4:
                        ghost_own[p] = ghost_own[p] + coef_own[p][d + 4:d + 5, :] * shifted[p]
                        ghost_face[p] = ghost_face[p] + coef_face[p][d + 4:d + 5, :] * shifted_own[p]
            for p in range(3):
                slope[0, f, p] = taps(F[p], in_ahead, in_behind) + taps(ghost_face[p], cross_ahead, cross_behind)
                radial = None
                for j in range(1, 5):
                    part = STENCIL[j - 1] * (face_pad[f, p, 8 + j:32 + j, :] - face_pad[f, p, 8 - j:32 - j, :])
                    radial = part if radial is None else radial + part
                slope[1, f, p] = radial
                slope[2, f, p] = azimuthal[p]
                own_fix[f, p] = taps(ghost_own[p], cross_ahead, cross_behind)
            return carry

        lax.fori_loop(0, 5, strip_slopes, 0)

        def fixed_by(ux, cut, scale):
            push = [cut[1], cut[4], None, None, cut[1]]
            return [-scale * (ux * cut[f] + push[f]) if push[f] is not None else -scale * (ux * cut[f]) for f in range(5)]

        for p in range(3):
            u = [flow_pack[m] for m in range(3)]
            dx, dr, da = ([slope[m, f, p] for f in range(5)] for m in range(3))
            push = forcing(dx, dr, da)
            for f in range(5):
                change = -(u[0] * dx[f] + u[1] * dr[f] + u[2] * da[f]) - push[f]
                face_mid[f, p] = face_pad[f, p, 8:32, :] + (0.5 * STEP_SIZE) * change
            fix = fixed_by(u[0], [own_fix[f, p] for f in range(5)], 0.5 * STEP_SIZE)
            for f in range(5):
                own_fix[f, p] = fix[f]

        near = (lane24 >= 60) & (lane24 < 68)

        def fix_mid(f, carry):
            for c in range(16):
                p, a = (c + 4) // 8, (c + 4) % 8
                wide = moved(own_fix[f, p], 16 * a - 56)
                mid[f, c, 8:32, :] = mid[f, c, 8:32, :] + jnp.where(near, wide, 0.0)
            ghosts = jnp.zeros((24, 128), F32)
            packs = [face_mid[f, p] for p in range(3)]
            for d in range(-4, 4):
                ghosts = ghosts + coef_own[1][d + 4:d + 5, :] * by_cells(packs, d, (1,))[0]
            slope[0, f, 0] = taps(ghosts, cross_ahead, cross_behind)
            return carry

        lax.fori_loop(0, 5, fix_mid, 0)
        fix = fixed_by(flow_pack[0], [slope[0, f, 0] for f in range(5)], STEP_SIZE)
        for f in range(5):
            slope[1, f, 0] = fix[f]

        def widen(f, carry):
            for a in range(8):
                fix_wide[f, a] = jnp.where(near, moved(slope[1, f, 0], 16 * a - 56), 0.0)
            return carry

        lax.fori_loop(0, 5, widen, 0)

        def second(c, carry):
            after = []
            for t in range(3):
                _, slopes = evaluate_rows(mid, c + 4, t)
                after.append([E[n, f, c + 8, 8 + 8 * t:16 + 8 * t, :] + STEP_SIZE * slopes[f]
                              + fix_wide[f, c, 8 * t:8 * t + 8, :] for f in range(5)])
            for t in range(2):
                for f in range(5):
                    own = jnp.where(r == 0, after[t][f], after[t + 1][f])
                    E[n + 1, f, c + 8, pl.ds(pl.multiple_of(row0 + 8 * t, 8), 8), :] = own
            return carry

        lax.fori_loop(0, 8, second, 0)
        for copy in started:
            copy.wait_send()

    for copy in fixed:
        copy.wait()
    for m in range(3):
        packed = None
        for a in range(8):
            turned = moved(flow[m], 56 - 16 * a)
            packed = turned if packed is None else jnp.where(lane24 // 16 == a, turned, packed)
        flow_pack[m] = packed

    step(0)
    step(1)
    store = pltpu.make_async_copy(E.at[2, :, pl.ds(8, 8), pl.ds(row0, 16), :], out_hbm, local_sem.at[0])
    store.start()
    store.wait()


def shards(acoustic_state, mean_flow, sector_offset, cell_shift, stencil_start, interface_fraction):
    smem = pl.BlockSpec(memory_space=pltpu.SMEM)
    anywhere = pl.BlockSpec(memory_space=pl.ANY)
    vmem = lambda *shape: pltpu.VMEM(shape, F32)
    return pl.pallas_call(
        kernel,
        out_shape=jax.ShapeDtypeStruct(acoustic_state.shape, F32),
        in_specs=[smem, smem, smem, smem, anywhere, anywhere],
        out_specs=anywhere,
        scratch_shapes=[
            vmem(3, 5, 24, 40, 128),
            vmem(5, 16, 40, 128),
            *[vmem(count, 11, 8, 128) for count in (2, NZ, NY, NX) for _ in range(2)],
            vmem(2, 3, 16, 8, 128),
            vmem(3, 2, 8, 128),
            vmem(3, 24, 128),
            vmem(3, 24, 128),
            vmem(5, 3, 24, 128),
            vmem(5, 3, 40, 128),
            vmem(3, 5, 3, 24, 128),
            vmem(5, 3, 24, 128),
            vmem(5, 3, 24, 128),
            vmem(5, 8, 24, 128),
            pltpu.SemaphoreType.DMA((2, 24)),
            pltpu.SemaphoreType.DMA((2, 24)),
            pltpu.SemaphoreType.DMA((3,)),
            pltpu.SemaphoreType.DMA((3,)),
            pltpu.SemaphoreType.DMA((2,)),
        ],
        compiler_params=pltpu.CompilerParams(collective_id=0, has_side_effects=True, vmem_limit_bytes=40 * 1024 * 1024),
        name="acoustic_steps",
    )(sector_offset, cell_shift, stencil_start, interface_fraction, mean_flow, acoustic_state)


def solution(mesh):
    return jax.shard_map(
        shards,
        mesh=mesh,
        in_specs=(
            P(None, "azim", "rad", None),
            P(None, "rad", None),
            P(),
            P(None, "azim"),
            P(None, "azim"),
            P(None, "azim"),
        ),
        out_specs=P(None, "azim", "rad", None),
        check_vma=False,
    )
```

```python
import jax
import jax.numpy as jnp
from jax import lax
from jax.experimental import pallas as pl
from jax.experimental.pallas import tpu as pltpu
from jax.sharding import PartitionSpec as P

STENCIL = (0.841570125482, -0.244678631765, 0.059463584768, -0.007650904064)
STEP_SIZE = 0.2
MESH = pl.DeviceIdType.MESH
F32 = jnp.float32

NZ, NY, NX = 8, 4, 2
N = 128


def lanes(rows=8):
    return lax.broadcasted_iota(jnp.int32, (rows, 128), 1)


def moved(value, by):
    return value if by % 128 == 0 else pltpu.roll(value, (-by) % 128, value.ndim - 1)


def forcing(dx, dr, da):
    spread = dx[1] + dr[2] + da[3]
    return [spread, dx[4], dr[4], da[4], spread]


def kernel(offset_hbm, shift_hbm, start_hbm, fraction_hbm, flow_hbm, state_hbm, out_hbm,
           offset_ref, shift_ref, start_ref, fraction_ref,
           E, mid, slot_a0, slot_a1, slot_z0, slot_z1, slot_y0, slot_y1, slot_x0, slot_x1, facing, own_coef, flow, flow_pack,
           own_pack, face_pad, slope, face_mid, own_fix, next_pack, fix_pad,
           send_sem, recv_sem, fixed_send, fixed_recv, local_sem):
    slots_a, slots_z, slots_y, slots_x = (slot_a0, slot_a1), (slot_z0, slot_z1), (slot_y0, slot_y1), (slot_x0, slot_x1)
    i = lax.axis_index("azim")
    r = lax.axis_index("rad")
    core, z, y, x = i % 2, (i // 2) % NZ, (i // 16) % NY, i // 64
    row0 = pl.multiple_of(8 + 8 * r, 8)
    far0 = pl.multiple_of(8 + 16 * r, 8)
    up, down = (i + 1) % N, (i + N - 1) % N

    def at(azim, rad=None):
        return {"azim": azim, "rad": r if rad is None else rad}

    def along_z(d):
        return i - 2 * z + 2 * ((z + d + NZ) % NZ)

    other = 1 - 2 * core
    near_to = [(i + other, 2 + core)]
    for d in (1, -1):
        near_to += [(along_z(d), 2 * (1 - d) + core), (along_z(d) + other, 2 * (1 - d) + core)]
    z_to = [(along_z(3), 0), (along_z(-3), 2)]
    y_to = [i - 16 * y + 16 * ((y + d) % NY) for d in (2, 1, 3)]
    x_to = (i + 64) % N

    loads = []

    def load(src, dst):
        copy = pltpu.make_async_copy(src, dst, local_sem.at[len(loads)])
        copy.start()
        loads.append(copy)

    load(state_hbm, E.at[0, :, pl.ds(8, 8), pl.ds(row0, 16), :])
    load(flow_hbm, flow.at[:, pl.ds(pl.multiple_of(8 * r, 8), 16), :])
    load(shift_hbm, shift_ref)
    load(start_hbm, start_ref)
    load(fraction_hbm, fraction_ref)
    load(offset_hbm, offset_ref)

    barrier = pltpu.get_barrier_semaphore()
    partners = [at(j) for j, _ in near_to] + [at(j) for j, _ in z_to] + [at(j) for j in y_to] + [at(x_to)]
    partners += [at(up), at(down), at(i, 1 - r), at(up, 1 - r), at(down, 1 - r)]
    for partner in partners:
        pl.semaphore_signal(barrier, inc=1, device_id=partner, device_id_type=MESH)

    edge = jnp.zeros((5, 16, 8, 128), F32)
    corner = jnp.zeros((5, 4, 8, 128), F32)
    for n in range(2):
        E[n, :, 4:20, 0:8, :] = edge
        E[n, :, 4:20, 32:40, :] = edge
        far_own = pl.multiple_of(24 - 16 * r, 8)
        E[n, :, 0:4, pl.ds(far_own, 8), :] = corner
        E[n, :, 20:24, pl.ds(far_own, 8), :] = corner
    for low in (0, 32):
        mid[:, :, low:low + 8, :] = edge
        face_pad[:, :, low:low + 8, :] = jnp.zeros((5, 2, 8, 128), F32)
        fix_pad[:, low:low + 8, :] = jnp.zeros((5, 8, 128), F32)

    lane = lanes()
    cell_of = lane // 16
    upper = lane % 16 >= 8
    row = lax.broadcasted_iota(jnp.int32, (8, 128), 0)

    def spread_cells(get):
        value = jnp.full((8, 128), get(0))
        for a in range(1, 8):
            value = jnp.where(cell_of == a, get(a), value)
        return value

    def weights(t, m):
        up_one, down_one, down_two = t + 1.0, t - 1.0, t - 2.0
        w = (-t * down_one * down_two / 6.0, up_one * down_one * down_two / 2.0,
             -up_one * t * down_two / 2.0, up_one * t * down_one / 6.0)
        value = jnp.zeros((8, 128), F32)
        for p in range(4):
            value = jnp.where(m == p, w[p], value)
        return value

    def pack_rows(n, t, f):
        rows = pl.ds(pl.multiple_of(row0 + 8 * t, 8), 8)
        packed = None
        for a in range(8):
            turned = moved(E[n, f, 8 + a, rows, :], 56 - 16 * a)
            packed = turned if packed is None else jnp.where(cell_of == a, turned, packed)
        return packed

    for copy in loads:
        copy.wait()
    for t in range(2):
        for f in range(5):
            slots_a[0][2 + core, t * 5 + f] = pack_rows(0, t, f)
    stator_t = spread_cells(lambda a: fraction_ref[0, a])
    rotor_t = spread_cells(lambda a: fraction_ref[1, a])
    for n in range(2):
        stator = weights(stator_t, row - spread_cells(lambda a: shift_ref[n, a] + start_ref[0, a] + 3))
        rotor = weights(rotor_t, row - spread_cells(lambda a: start_ref[1, a] - shift_ref[n, a]))
        own_coef[1, n] = jnp.where(upper, stator, rotor)
        slots_a[n][2 + core, 10] = jnp.where(upper, rotor, stator)

    pl.semaphore_wait(barrier, len(partners))
    fixed = []

    def send_fixed(src, dst, to):
        no = len(fixed)
        copy = pltpu.make_async_remote_copy(src, dst, fixed_send.at[no], fixed_recv.at[no], device_id=to, device_id_type=MESH)
        copy.start()
        fixed.append(copy)

    half = lane % 64
    strip = lane % 16
    ahead = [jnp.where(half + j < 64, STENCIL[j - 1], 0.0) for j in range(1, 5)]
    behind = [jnp.where(half - j >= 0, STENCIL[j - 1], 0.0) for j in range(1, 5)]

    def tall(v):
        return jnp.concatenate([v, v, v], axis=0)

    in_ahead = [tall(jnp.where(strip % 8 + j < 8, STENCIL[j - 1], 0.0)) for j in range(1, 5)]
    in_behind = [tall(jnp.where(strip % 8 - j >= 0, STENCIL[j - 1], 0.0)) for j in range(1, 5)]
    cross_ahead = [tall(jnp.where((strip < 8) & (strip + j >= 8), STENCIL[j - 1], 0.0)) for j in range(1, 5)]
    cross_behind = [tall(jnp.where((strip >= 8) & (strip - j < 8), STENCIL[j - 1], 0.0)) for j in range(1, 5)]
    lane24 = lanes(24)

    def taps(value, fore, aft):
        total = None
        for j in range(1, 5):
            term = fore[j - 1] * moved(value, j) - aft[j - 1] * moved(value, -j)
            total = term if total is None else total + term
        return total

    def ring(sectors):
        turned = [moved(v, 64) for v in sectors]
        low = lanes(turned[0].shape[0]) < 64
        return [jnp.where(low, turned[p], turned[(p + 1) % 3]) for p in range(3)]

    def by_cells(packs, d):
        if d == 0:
            return packs[:2]
        turned = [moved(v, 16 * d) for v in packs]
        if d > 0:
            return [jnp.where(lane24 < 128 - 16 * d, turned[p], turned[p + 1]) for p in range(2)]
        return [jnp.where(lane24 >= -16 * d, turned[p], turned[(p + 2) % 3]) for p in range(2)]

    def between(packs, o):
        if o % 8 == 0:
            return packs[o // 8]
        return jnp.where(lane24 < 128 - 16 * o, moved(packs[0], 16 * o), moved(packs[1], 16 * o))

    def evaluate_rows(ref, c, t):
        low = 8 + 8 * t
        dx, dr, da, mine = [], [], [], []
        for f in range(5):
            here = ref[f, c, low:low + 8, :]
            mine.append(here)
            dx.append(taps(here, ahead, behind))
            radial = azimuthal = None
            for j in range(1, 5):
                step = STENCIL[j - 1] * (ref[f, c, low + j:low + j + 8, :] - ref[f, c, low - j:low - j + 8, :])
                radial = step if radial is None else radial + step
                step = STENCIL[j - 1] * (ref[f, c + j, low:low + 8, :] - ref[f, c - j, low:low + 8, :])
                azimuthal = step if azimuthal is None else azimuthal + step
            dr.append(radial)
            da.append(azimuthal)
        u = [flow[k, 8 * t:8 * t + 8, :] for k in range(3)]
        push = forcing(dx, dr, da)
        return mine, [-(u[0] * dx[f] + u[1] * dr[f] + u[2] * da[f]) - push[f] for f in range(5)]

    def radial_of(ref, *index):
        total = None
        for j in range(1, 5):
            part = STENCIL[j - 1] * (ref[(*index, slice(8 + j, 32 + j))] - ref[(*index, slice(8 - j, 32 - j))])
            total = part if total is None else total + part
        return total

    def own_rows_of(value, t):
        return jnp.where(r == 0, value[8 * t:8 * t + 8], value[8 * t + 8:8 * t + 16])

    def step(n):
        slot_a, slot_z, slot_y, slot_x = slots_a[n], slots_z[n], slots_y[n], slots_x[n]
        k = offset_ref[n]
        source_r = (i - k + N) % N
        source_s = (i + k) % N
        low_r = (core - k % 16 + 16) % 16
        low_s = (core + k % 16) % 16
        started = []

        def parts(low):
            far = ((low // 2 + 3) % 8 + 1) // 3 - 1
            near = (low // 2 + 3) % 8 - 3 - 3 * far
            return near, far

        def send(src, dst, to):
            no = len(started)
            copy = pltpu.make_async_remote_copy(src, dst, send_sem.at[n, no], recv_sem.at[n, no], device_id=to, device_id_type=MESH)
            copy.start()
            started.append(copy)
            return copy

        def chosen(slots, from_r, from_s):
            return jnp.where(upper[None], slots[from_r], slots[from_s])

        mine = slot_a.at[2 + core]
        stage = [send(mine, slot_a.at[place], at(j)) for j, place in near_to]

        if n == 0:
            send_fixed(own_coef.at[1], own_coef.at[0], at(up))
            send_fixed(own_coef.at[1], own_coef.at[2], at(down))
            send_fixed(flow.at[:, pl.ds(8, 8), :], flow.at[:, pl.ds(pl.multiple_of(16 * r, 8), 8), :], at(i, 1 - r))
        else:
            def into_rows(f, carry):
                for t in range(2):
                    change = own_rows_of(own_fix[f, 0], t)
                    rows = pl.ds(pl.multiple_of(row0 + 8 * t, 8), 8)
                    for a in range(8):
                        E[1, f, 8 + a, rows, :] = E[1, f, 8 + a, rows, :] + jnp.where(
                            (lane >= 56) & (lane < 72), moved(change, 16 * a - 56), 0.0)
                return carry

            lax.fori_loop(0, 5, into_rows, 0)

        own_rows, far_rows = pl.ds(row0, 16), pl.ds(far0, 8)
        halos = []
        halos.append(send(E.at[n, :, pl.ds(8, 8), pl.ds(16, 8), :], E.at[n, :, pl.ds(8, 8), far_rows, :], at(i, 1 - r)))
        halos.append(send(E.at[n, :, pl.ds(12, 4), pl.ds(16, 8), :], E.at[n, :, pl.ds(4, 4), far_rows, :], at(up, 1 - r)))
        halos.append(send(E.at[n, :, pl.ds(8, 4), pl.ds(16, 8), :], E.at[n, :, pl.ds(16, 4), far_rows, :], at(down, 1 - r)))
        for copy in stage:
            copy.wait_recv()

        (near_r, far_r), (near_s, far_s) = parts(low_r), parts(low_s)
        slot_z[1] = chosen(slot_a, 2 * (near_r + 1) + low_r % 2, 2 * (near_s + 1) + low_s % 2)
        mine = slot_z.at[1]
        stage = [send(mine, slot_z.at[place], at(j)) for j, place in z_to]
        halos.append(send(E.at[n, :, pl.ds(8, 8), own_rows, :], E.at[n, :, pl.ds(0, 8), own_rows, :], at(up)))
        halos.append(send(E.at[n, :, pl.ds(8, 8), own_rows, :], E.at[n, :, pl.ds(16, 8), own_rows, :], at(down)))
        for copy in stage:
            copy.wait_recv()

        slot_y[y] = chosen(slot_z, far_r + 1, far_s + 1)
        mine = slot_y.at[y]
        stage = [send(mine, mine, at(j)) for j in y_to]
        for copy in stage:
            copy.wait_recv()

        slot_x[x] = chosen(slot_y, (source_r // 16) % NY, (source_s // 16) % NY)
        mine = slot_x.at[x]
        stage = [send(mine, mine, at(x_to))]

        if n == 0:
            for copy in fixed:
                copy.wait()
            for m in range(3):
                packed = None
                for a in range(8):
                    turned = moved(flow[m], 56 - 16 * a)
                    packed = turned if packed is None else jnp.where(lane24 // 16 == a, turned, packed)
                flow_pack[m] = packed
        for copy in halos:
            copy.wait_recv()

        def first(c, carry):
            for t in range(3):
                here, slopes = evaluate_rows(E.at[n], c + 4, t)
                for f in range(5):
                    mid[f, c, 8 + 8 * t:16 + 8 * t, :] = here[f] + (0.5 * STEP_SIZE) * slopes[f]
            return carry

        lax.fori_loop(0, 16, first, 0)
        for copy in stage:
            copy.wait_recv()

        got = chosen(slot_x, source_r // 64, source_s // 64)
        facing[n, 1, pl.ds(5 * r, 10)] = got[0:10]
        facing[n, 1, 15] = got[10]
        rows10, rows5 = pl.ds(5 * r, 10), pl.ds(10 * r, 5)
        stage = []
        for to, place in ((up, 0), (down, 2)):
            stage.append(send(facing.at[n, 1, rows10], facing.at[n, place, rows10], at(to)))
            stage.append(send(facing.at[n, 1, 15], facing.at[n, place, 15], at(to)))
            stage.append(send(facing.at[n, 1, pl.ds(5, 5)], facing.at[n, place, rows5], at(to, 1 - r)))
        stage.append(send(facing.at[n, 1, pl.ds(5, 5)], facing.at[n, 1, rows5], at(i, 1 - r)))

        def second(c, carry):
            after = []
            for t in range(3):
                _, slopes = evaluate_rows(mid, c + 4, t)
                after.append([E[n, f, c + 8, 8 + 8 * t:16 + 8 * t, :] + STEP_SIZE * slopes[f] for f in range(5)])
            for t in range(2):
                for f in range(5):
                    own = jnp.where(r == 0, after[t][f], after[t + 1][f])
                    E[n + 1, f, c + 8, pl.ds(pl.multiple_of(row0 + 8 * t, 8), 8), :] = own
            return carry

        lax.fori_loop(0, 8, second, 0)

        def strip_of(f, carry):
            for p in range(3):
                packed = None
                for a in range(8):
                    turned = moved(E[n, f, (4 + 8 * p + a) % 24, 8:32, :], 56 - 16 * a)
                    packed = turned if packed is None else jnp.where(lane24 // 16 == a, turned, packed)
                own_pack[f, p] = packed
            if n == 0:
                for t in range(2):
                    next_pack[t, f] = pack_rows(1, t, f)
            return carry

        lax.fori_loop(0, 5, strip_of, 0)
        coef_own = ring([own_coef[p, n] for p in range(3)])
        for copy in stage:
            copy.wait_recv()

        coef_face = ring([jnp.where(upper, moved(facing[n, p, 15], -8), moved(facing[n, p, 15], 8)) for p in range(3)])

        def strip_slopes(f, carry):
            F = ring([jnp.concatenate([facing[n, p, 5 * t + f] for t in range(3)], axis=0) for p in range(3)])
            M = [own_pack[f, p] for p in range(3)]
            for p in range(2):
                face_pad[f, p, 8:32, :] = F[p]
            ghost_own = [jnp.zeros((24, 128), F32)] * 2
            ghost_face = [jnp.zeros((24, 128), F32)] * 2
            azimuthal = [jnp.zeros((24, 128), F32)] * 2
            for d in range(-4, 5):
                shifted = by_cells(F, d)
                if d < 4:
                    shifted_own = by_cells(M, d)
                for p in range(2):
                    if d != 0:
                        weight = STENCIL[d - 1] if d > 0 else -STENCIL[-d - 1]
                        azimuthal[p] = azimuthal[p] + weight * shifted[p]
                    if d < 4:
                        ghost_own[p] = ghost_own[p] + coef_own[p][d + 4:d + 5, :] * shifted[p]
                        ghost_face[p] = ghost_face[p] + coef_face[p][d + 4:d + 5, :] * shifted_own[p]
            for p in range(2):
                slope[0, f, p] = taps(F[p], in_ahead, in_behind) + taps(ghost_face[p], cross_ahead, cross_behind)
                slope[1, f, p] = radial_of(face_pad, f, p)
                slope[2, f, p] = azimuthal[p]
                own_fix[f, p] = taps(ghost_own[p], cross_ahead, cross_behind)
            return carry

        lax.fori_loop(0, 5, strip_slopes, 0)

        u = [flow_pack[m] for m in range(3)]
        for p in range(2):
            dx, dr, da = ([slope[m, f, p] for f in range(5)] for m in range(3))
            push = forcing(dx, dr, da)
            for f in range(5):
                change = -(u[0] * dx[f] + u[1] * dr[f] + u[2] * da[f]) - push[f]
                face_mid[f, p] = face_pad[f, p, 8:32, :] + (0.5 * STEP_SIZE) * change
            cut = [own_fix[f, p] for f in range(5)]
            push = [cut[1], cut[4], 0.0, 0.0, cut[1]]
            for f in range(5):
                own_fix[f, p] = (-0.5 * STEP_SIZE) * (u[0] * cut[f] + push[f])

        def fix_slopes(f, carry):
            face = [face_mid[f, p] for p in range(2)]
            fix = [own_fix[f, p] for p in range(2)]
            ghosts = jnp.zeros((24, 128), F32)
            azimuthal = jnp.zeros((24, 128), F32)
            for o in range(9):
                if o < 8:
                    ghosts = ghosts + own_coef[1, n, o:o + 1, :] * between(face, o)
                if o != 4:
                    weight = STENCIL[o - 5] if o > 4 else -STENCIL[3 - o]
                    azimuthal = azimuthal + weight * between(fix, o)
            here = between(fix, 4)
            fix_pad[f, 8:32, :] = here
            slope[0, f, 0] = taps(here, in_ahead, in_behind) + taps(ghosts, cross_ahead, cross_behind)
            slope[1, f, 0] = radial_of(fix_pad, f)
            slope[2, f, 0] = azimuthal
            return carry

        lax.fori_loop(0, 5, fix_slopes, 0)
        dx, dr, da = ([slope[m, f, 0] for f in range(5)] for m in range(3))
        push = forcing(dx, dr, da)
        for f in range(5):
            change = -STEP_SIZE * (u[0] * dx[f] + u[1] * dr[f] + u[2] * da[f] + push[f])
            own_fix[f, 0] = change
            if n == 0:
                for t in range(2):
                    slots_a[1][2 + core, 5 * t + f] = next_pack[t, f] + own_rows_of(change, t)
        return started

    started = step(0)
    started += step(1)

    def into_result(f, carry):
        for t in range(2):
            change = own_rows_of(own_fix[f, 0], t)
            rows = pl.ds(pl.multiple_of(row0 + 8 * t, 8), 8)
            for a in range(8):
                E[2, f, 8 + a, rows, :] = E[2, f, 8 + a, rows, :] + jnp.where(
                    (lane >= 56) & (lane < 72), moved(change, 16 * a - 56), 0.0)
        return carry

    lax.fori_loop(0, 5, into_result, 0)
    store = pltpu.make_async_copy(E.at[2, :, pl.ds(8, 8), pl.ds(row0, 16), :], out_hbm, local_sem.at[0])
    store.start()
    for copy in started:
        copy.wait_send()
    store.wait()


def shards(acoustic_state, mean_flow, sector_offset, cell_shift, stencil_start, interface_fraction):
    anywhere = pl.BlockSpec(memory_space=pl.ANY)
    vmem = lambda *shape: pltpu.VMEM(shape, F32)
    smem = lambda value: pltpu.SMEM(value.shape, value.dtype)
    return pl.pallas_call(
        kernel,
        out_shape=jax.ShapeDtypeStruct(acoustic_state.shape, F32),
        in_specs=[anywhere] * 6,
        out_specs=anywhere,
        scratch_shapes=[
            smem(sector_offset),
            smem(cell_shift),
            smem(stencil_start),
            smem(interface_fraction),
            vmem(3, 5, 24, 40, 128),
            vmem(5, 16, 40, 128),
            *[vmem(count, 11, 8, 128) for count in (6, 3, NY, NX) for _ in range(2)],
            vmem(2, 3, 16, 8, 128),
            vmem(3, 2, 8, 128),
            vmem(3, 24, 128),
            vmem(3, 24, 128),
            vmem(5, 3, 24, 128),
            vmem(5, 2, 40, 128),
            vmem(3, 5, 2, 24, 128),
            vmem(5, 2, 24, 128),
            vmem(5, 2, 24, 128),
            vmem(2, 5, 8, 128),
            vmem(5, 40, 128),
            pltpu.SemaphoreType.DMA((2, 24)),
            pltpu.SemaphoreType.DMA((2, 24)),
            pltpu.SemaphoreType.DMA((3,)),
            pltpu.SemaphoreType.DMA((3,)),
            pltpu.SemaphoreType.DMA((6,)),
        ],
        compiler_params=pltpu.CompilerParams(collective_id=0, has_side_effects=True, vmem_limit_bytes=67043328),
        name="acoustic_steps",
    )(sector_offset, cell_shift, stencil_start, interface_fraction, mean_flow, acoustic_state)


def solution(mesh):
    return jax.shard_map(
        shards,
        mesh=mesh,
        in_specs=(
            P(None, "azim", "rad", None),
            P(None, "rad", None),
            P(),
            P(None, "azim"),
            P(None, "azim"),
            P(None, "azim"),
        ),
        out_specs=P(None, "azim", "rad", None),
        check_vma=False,
    )
```

```python
import jax
import jax.numpy as jnp
from jax import lax
from jax.experimental import pallas as pl
from jax.experimental.pallas import tpu as pltpu
from jax.sharding import PartitionSpec as P

STENCIL = (0.841570125482, -0.244678631765, 0.059463584768, -0.007650904064)
STEP_SIZE = 0.2
MESH = pl.DeviceIdType.MESH
F32 = jnp.float32

NZ, NY, NX = 8, 4, 2
N = 128


def lanes(rows=8):
    return lax.broadcasted_iota(jnp.int32, (rows, 128), 1)


def moved(value, by):
    return value if by % 128 == 0 else pltpu.roll(value, (-by) % 128, value.ndim - 1)


def forcing(dx, dr, da):
    spread = dx[1] + dr[2] + da[3]
    return [spread, dx[4], dr[4], da[4], spread]


def kernel(offset_hbm, shift_hbm, start_hbm, fraction_hbm, flow_hbm, state_hbm, out_hbm, fix_hbm,
           offset_ref, shift_ref, start_ref, fraction_ref,
           E, mid, slot_a0, slot_a1, slot_z0, slot_z1, slot_y0, slot_y1, slot_x0, slot_x1, facing, own_coef, flow, flow_pack,
           own_pack, face_pad, slope, face_mid, own_fix, next_pack, fix_pad, wide_fix,
           send_sem, recv_sem, fixed_send, fixed_recv, local_sem):
    slots_a, slots_z, slots_y, slots_x = (slot_a0, slot_a1), (slot_z0, slot_z1), (slot_y0, slot_y1), (slot_x0, slot_x1)
    i = lax.axis_index("azim")
    r = lax.axis_index("rad")
    core, z, y, x = i % 2, (i // 2) % NZ, (i // 16) % NY, i // 64
    row0 = pl.multiple_of(8 + 8 * r, 8)
    far0 = pl.multiple_of(8 + 16 * r, 8)
    far0_here = pl.multiple_of(24 - 16 * r, 8)
    up, down = (i + 1) % N, (i + N - 1) % N

    def at(azim, rad=None):
        return {"azim": azim, "rad": r if rad is None else rad}

    def along_z(d):
        return i - 2 * z + 2 * ((z + d + NZ) % NZ)

    other = 1 - 2 * core
    near_to = [(i + other, 2 + core)]
    for d in (1, -1):
        near_to += [(along_z(d), 2 * (1 - d) + core), (along_z(d) + other, 2 * (1 - d) + core)]
    z_to = [(along_z(3), 0), (along_z(-3), 2)]
    y_to = [i - 16 * y + 16 * ((y + d) % NY) for d in (2, 1, 3)]
    x_to = (i + 64) % N

    loads = []

    def load(src, dst):
        copy = pltpu.make_async_copy(src, dst, local_sem.at[len(loads)])
        copy.start()
        loads.append(copy)

    load(state_hbm, E.at[0, :, pl.ds(8, 8), pl.ds(row0, 16), :])
    load(flow_hbm, flow.at[:, pl.ds(pl.multiple_of(8 * r, 8), 16), :])
    load(shift_hbm, shift_ref)
    load(start_hbm, start_ref)
    load(fraction_hbm, fraction_ref)
    load(offset_hbm, offset_ref)

    barrier = pltpu.get_barrier_semaphore()
    partners = [at(j) for j, _ in near_to] + [at(j) for j, _ in z_to] + [at(j) for j in y_to] + [at(x_to)]
    partners += [at(up), at(down), at(i, 1 - r), at(up, 1 - r), at(down, 1 - r)]
    for partner in partners:
        pl.semaphore_signal(barrier, inc=1, device_id=partner, device_id_type=MESH)

    edge = jnp.zeros((5, 16, 8, 128), F32)
    for n in range(2):
        E[n, :, 4:20, 0:8, :] = edge
        E[n, :, 4:20, 32:40, :] = edge
    for low in (0, 32):
        mid[:, :, low:low + 8, :] = edge
        face_pad[:, :, low:low + 8, :] = jnp.zeros((5, 2, 8, 128), F32)
        fix_pad[:, low:low + 8, :] = jnp.zeros((5, 8, 128), F32)

    lane = lanes()
    cell_of = (lane // 16 + 4) % 8
    upper = lane % 16 >= 8
    row = lax.broadcasted_iota(jnp.int32, (8, 128), 0)

    def spread_cells(get):
        value = jnp.full((8, 128), get(0))
        for a in range(1, 8):
            value = jnp.where(cell_of == a, get(a), value)
        return value

    def weights(t, m):
        up_one, down_one, down_two = t + 1.0, t - 1.0, t - 2.0
        w = (-t * down_one * down_two / 6.0, up_one * down_one * down_two / 2.0,
             -up_one * t * down_two / 2.0, up_one * t * down_one / 6.0)
        value = jnp.zeros((8, 128), F32)
        for p in range(4):
            value = jnp.where(m == p, w[p], value)
        return value

    def pack_rows(n, t, f):
        rows = pl.ds(pl.multiple_of(row0 + 8 * t, 8), 8)
        packed = None
        for a in range(8):
            turned = moved(E[n, f, 8 + a, rows, :], 56 - 16 * ((a + 4) % 8))
            packed = turned if packed is None else jnp.where(cell_of == a, turned, packed)
        return packed

    for copy in loads:
        copy.wait()
    for t in range(2):
        for f in range(5):
            slots_a[0][2 + core, t * 5 + f] = pack_rows(0, t, f)
    stator_t = spread_cells(lambda a: fraction_ref[0, a])
    rotor_t = spread_cells(lambda a: fraction_ref[1, a])
    for n in range(2):
        stator = weights(stator_t, row - spread_cells(lambda a: shift_ref[n, a] + start_ref[0, a] + 3))
        rotor = weights(rotor_t, row - spread_cells(lambda a: start_ref[1, a] - shift_ref[n, a]))
        own_coef[1, n] = jnp.where(upper, stator, rotor)
        slots_a[n][2 + core, 10] = jnp.where(upper, rotor, stator)

    pl.semaphore_wait(barrier, len(partners))
    fixed = []

    def send_fixed(src, dst, to):
        no = len(fixed)
        copy = pltpu.make_async_remote_copy(src, dst, fixed_send.at[no], fixed_recv.at[no], device_id=to, device_id_type=MESH)
        copy.start()
        fixed.append(copy)

    half = lane % 64
    strip = lane % 16
    ahead = [jnp.where(half + j < 64, STENCIL[j - 1], 0.0) for j in range(1, 5)]
    behind = [jnp.where(half - j >= 0, STENCIL[j - 1], 0.0) for j in range(1, 5)]

    in_ahead = [jnp.where(strip % 8 + j < 8, STENCIL[j - 1], 0.0) for j in range(1, 5)]
    in_behind = [jnp.where(strip % 8 - j >= 0, STENCIL[j - 1], 0.0) for j in range(1, 5)]
    cross_ahead = [jnp.where((strip < 8) & (strip + j >= 8), STENCIL[j - 1], 0.0) for j in range(1, 5)]
    cross_behind = [jnp.where((strip >= 8) & (strip - j < 8), STENCIL[j - 1], 0.0) for j in range(1, 5)]

    def taps(value, fore, aft):
        total = None
        for j in range(1, 5):
            term = fore[j - 1][0:1] * moved(value, j) - aft[j - 1][0:1] * moved(value, -j)
            total = term if total is None else total + term
        return total

    def ring(sectors):
        low = lanes(sectors[0].shape[0]) < 64
        return [jnp.where(low, sectors[p], sectors[(p + 1) % 3]) for p in range(3)]

    def by_cells(packs, d):
        if d == 0:
            return packs[:2]
        at_lane = lanes(packs[0].shape[0])
        turned = [moved(v, 16 * d) for v in packs]
        if d > 0:
            return [jnp.where(at_lane < 128 - 16 * d, turned[p], turned[p + 1]) for p in range(2)]
        return [jnp.where(at_lane >= -16 * d, turned[p], turned[(p + 2) % 3]) for p in range(2)]

    def own_cells(packs, d):
        at_lane = lanes(packs[0].shape[0])
        first, last = (moved(v, 16 * d) for v in packs)
        if d >= 0:
            return jnp.where((at_lane >= 64) & (at_lane < 128 - 16 * d), first, last)
        return jnp.where((at_lane < 64) & (at_lane >= -16 * d), last, first)

    def evaluate_rows(ref, c, low):
        dx, dr, da, mine = [], [], [], []
        rows = pl.ds(low, 8)
        for f in range(5):
            here = ref[f, c, rows, :]
            mine.append(here)
            dx.append(taps(here, ahead, behind))
            radial = azimuthal = None
            for j in range(1, 5):
                step = STENCIL[j - 1] * (ref[f, c, pl.ds(low + j, 8), :] - ref[f, c, pl.ds(low - j, 8), :])
                radial = step if radial is None else radial + step
                step = STENCIL[j - 1] * (ref[f, c + j, rows, :] - ref[f, c - j, rows, :])
                azimuthal = step if azimuthal is None else azimuthal + step
            dr.append(radial)
            da.append(azimuthal)
        u = [flow[k, pl.ds(pl.multiple_of(low - 8, 8), 8), :] for k in range(3)]
        push = forcing(dx, dr, da)
        return mine, [-(u[0] * dx[f] + u[1] * dr[f] + u[2] * da[f]) - push[f] for f in range(5)]

    def radial_of(ref, *index):
        total = None
        for j in range(1, 5):
            part = STENCIL[j - 1] * (ref[(*index, slice(8 + j, 32 + j))] - ref[(*index, slice(8 - j, 32 - j))])
            total = part if total is None else total + part
        return total

    def own_rows_of(value):
        return jnp.where(r == 0, value[0:16], value[8:24])

    def widened(f, t, a):
        change = own_fix[f, 0, 8 * t:8 * t + 8, :]
        return jnp.where((lane >= 56) & (lane < 72), moved(change, 16 * ((a + 4) % 8) - 56), 0.0)

    def step(n):
        slot_a, slot_z, slot_y, slot_x = slots_a[n], slots_z[n], slots_y[n], slots_x[n]
        k = offset_ref[n]
        source_r = (i - k + N) % N
        source_s = (i + k) % N
        low_r = (core - k % 16 + 16) % 16
        low_s = (core + k % 16) % 16
        started = []

        def parts(low):
            far = ((low // 2 + 3) % 8 + 1) // 3 - 1
            near = (low // 2 + 3) % 8 - 3 - 3 * far
            return near, far

        def send(src, dst, to):
            no = len(started)
            copy = pltpu.make_async_remote_copy(src, dst, send_sem.at[n, no], recv_sem.at[n, no], device_id=to, device_id_type=MESH)
            copy.start()
            started.append(copy)
            return copy

        def chosen(slots, from_r, from_s):
            return jnp.where(upper[None], slots[from_r], slots[from_s])

        mine = slot_a.at[2 + core]
        stage = [send(mine, slot_a.at[place], at(j)) for j, place in near_to]

        if n == 0:
            send_fixed(own_coef.at[1], own_coef.at[0], at(up))
            send_fixed(own_coef.at[1], own_coef.at[2], at(down))
            send_fixed(flow.at[:, pl.ds(8, 8), :], flow.at[:, pl.ds(pl.multiple_of(16 * r, 8), 8), :], at(i, 1 - r))
        else:
            def into_rows(f, carry):
                for t in range(2):
                    rows = pl.ds(pl.multiple_of(row0 + 8 * t, 8), 8)
                    for a in range(8):
                        E[1, f, 8 + a, rows, :] = E[1, f, 8 + a, rows, :] + widened(f, t, a)
                return carry

            lax.fori_loop(0, 5, into_rows, 0)

        own_rows, far_rows = pl.ds(row0, 16), pl.ds(far0, 8)
        halos = []
        halos.append(send(E.at[n, :, pl.ds(8, 8), pl.ds(16, 8), :], E.at[n, :, pl.ds(8, 8), far_rows, :], at(i, 1 - r)))
        halos.append(send(E.at[n, :, pl.ds(12, 4), pl.ds(16, 8), :], E.at[n, :, pl.ds(4, 4), far_rows, :], at(up, 1 - r)))
        halos.append(send(E.at[n, :, pl.ds(8, 4), pl.ds(16, 8), :], E.at[n, :, pl.ds(16, 4), far_rows, :], at(down, 1 - r)))
        for copy in stage:
            copy.wait_recv()

        (near_r, far_r), (near_s, far_s) = parts(low_r), parts(low_s)
        slot_z[1] = chosen(slot_a, 2 * (near_r + 1) + low_r % 2, 2 * (near_s + 1) + low_s % 2)
        mine = slot_z.at[1]
        stage = [send(mine, slot_z.at[place], at(j)) for j, place in z_to]
        halos.append(send(E.at[n, :, pl.ds(8, 8), own_rows, :], E.at[n, :, pl.ds(0, 8), own_rows, :], at(up)))
        halos.append(send(E.at[n, :, pl.ds(8, 8), own_rows, :], E.at[n, :, pl.ds(16, 8), own_rows, :], at(down)))
        for copy in stage:
            copy.wait_recv()

        slot_y[y] = chosen(slot_z, far_r + 1, far_s + 1)
        mine = slot_y.at[y]
        stage = [send(mine, mine, at(j)) for j in y_to]
        for copy in stage:
            copy.wait_recv()

        slot_x[x] = chosen(slot_y, (source_r // 16) % NY, (source_s // 16) % NY)
        mine = slot_x.at[x]
        stage = [send(mine, mine, at(x_to))]

        if n == 0:
            for copy in fixed:
                copy.wait()
            for m in range(3):
                packed = None
                for a in range(8):
                    turned = moved(flow[m], 56 - 16 * a)
                    packed = turned if packed is None else jnp.where(lanes(24) // 16 == a, turned, packed)
                flow_pack[m] = packed
        for copy in halos:
            copy.wait_recv()

        def midpoint(c, low):
            here, slopes = evaluate_rows(E.at[n], c + 4, low)
            for f in range(5):
                mid[f, c, pl.ds(low, 8), :] = here[f] + (0.5 * STEP_SIZE) * slopes[f]

        def first(c, carry):
            midpoint(c, row0)
            midpoint(c, pl.multiple_of(row0 + 8, 8))
            return carry

        def first_far(c, carry):
            midpoint(c + 4, far0_here)
            return carry

        lax.fori_loop(0, 16, first, 0)
        lax.fori_loop(0, 8, first_far, 0)
        for copy in stage:
            copy.wait_recv()

        got = chosen(slot_x, source_r // 64, source_s // 64)
        facing[n, 1, pl.ds(5 * r, 10)] = got[0:10]
        facing[n, 1, 15] = got[10]
        rows10, rows5 = pl.ds(5 * r, 10), pl.ds(10 * r, 5)
        stage = []
        for to, place in ((up, 0), (down, 2)):
            stage.append(send(facing.at[n, 1, rows10], facing.at[n, place, rows10], at(to)))
            stage.append(send(facing.at[n, 1, 15], facing.at[n, place, 15], at(to)))
            stage.append(send(facing.at[n, 1, pl.ds(5, 5)], facing.at[n, place, rows5], at(to, 1 - r)))
        stage.append(send(facing.at[n, 1, pl.ds(5, 5)], facing.at[n, 1, rows5], at(i, 1 - r)))

        def second(c, carry):
            for t in range(2):
                low = pl.multiple_of(row0 + 8 * t, 8)
                _, slopes = evaluate_rows(mid, c + 4, low)
                for f in range(5):
                    E[n + 1, f, c + 8, pl.ds(low, 8), :] = E[n, f, c + 8, pl.ds(low, 8), :] + STEP_SIZE * slopes[f]
            return carry

        lax.fori_loop(0, 8, second, 0)
        if n == 1:
            pltpu.make_async_copy(*result, local_sem.at[0]).start()

        def strip_of(f, carry):
            for p in range(3):
                packed = None
                for a in range(8):
                    turned = moved(E[n, f, (4 + 8 * p + a) % 24, own_rows, :], 56 - 16 * a)
                    packed = turned if packed is None else jnp.where(lanes(16) // 16 == a, turned, packed)
                own_pack[f, p] = packed
            if n == 0:
                for t in range(2):
                    next_pack[f, 8 * t:8 * t + 8, :] = pack_rows(1, t, f)
            return carry

        lax.fori_loop(0, 5, strip_of, 0)
        coef_own = ring([own_coef[p, n] for p in range(3)])
        u24 = [flow_pack[m] for m in range(3)]
        u = [flow_pack[m, pl.ds(pl.multiple_of(8 * r, 8), 16), :] for m in range(3)]
        for copy in stage:
            copy.wait_recv()

        coef_face = ring([jnp.where(upper, moved(facing[n, p, 15], -8), moved(facing[n, p, 15], 8)) for p in range(3)])

        for f in range(5):
            F = ring([jnp.concatenate([facing[n, p, 5 * t + f] for t in range(3)], axis=0) for p in range(3)])
            M = [own_pack[f, p] for p in range(3)]
            F_own = [own_rows_of(v) for v in F]
            for p in range(2):
                face_pad[f, p, 8:32, :] = F[p]
            ghost_own = [jnp.zeros((24, 128), F32)] * 2
            ghost_face = [jnp.zeros((16, 128), F32)] * 2
            azimuthal = [jnp.zeros((16, 128), F32)] * 2
            for d in range(-4, 5):
                shifted = by_cells(F if d < 4 else F_own, d)
                if d < 4:
                    shifted_own = by_cells(M, d)
                for p in range(2):
                    if d != 0:
                        weight = STENCIL[d - 1] if d > 0 else -STENCIL[-d - 1]
                        azimuthal[p] = azimuthal[p] + weight * (own_rows_of(shifted[p]) if d < 4 else shifted[p])
                    if d < 4:
                        ghost_own[p] = ghost_own[p] + coef_own[p][d + 4:d + 5, :] * shifted[p]
                        ghost_face[p] = ghost_face[p] + coef_face[p][d + 4:d + 5, :] * shifted_own[p]
            for p in range(2):
                slope[0, f, p] = taps(F_own[p], in_ahead, in_behind) + taps(ghost_face[p], cross_ahead, cross_behind)
                slope[1, f, p] = own_rows_of(radial_of(face_pad, f, p))
                slope[2, f, p] = azimuthal[p]
                own_fix[f, p] = taps(ghost_own[p], cross_ahead, cross_behind)

        for p in range(2):
            dx, dr, da = ([slope[m, f, p] for f in range(5)] for m in range(3))
            push = forcing(dx, dr, da)
            for f in range(5):
                change = -(u[0] * dx[f] + u[1] * dr[f] + u[2] * da[f]) - push[f]
                face_mid[f, p] = face_pad[f, p, own_rows, :] + (0.5 * STEP_SIZE) * change
            cut = [own_fix[f, p] for f in range(5)]
            push = [cut[1], cut[4], 0.0, 0.0, cut[1]]
            for f in range(5):
                own_fix[f, p] = (-0.5 * STEP_SIZE) * (u24[0] * cut[f] + push[f])

        for f in range(5):
            face = [face_mid[f, p] for p in range(2)]
            fix = [own_rows_of(own_fix[f, p]) for p in range(2)]
            fix_pad[f, 8:32, :] = own_cells([own_fix[f, p] for p in range(2)], 0)
            ghosts = jnp.zeros((16, 128), F32)
            azimuthal = jnp.zeros((16, 128), F32)
            for d in range(-4, 5):
                if d < 4:
                    ghosts = ghosts + own_coef[1, n, d + 4:d + 5, :] * own_cells(face, d)
                if d != 0:
                    weight = STENCIL[d - 1] if d > 0 else -STENCIL[-d - 1]
                    azimuthal = azimuthal + weight * own_cells(fix, d)
            slope[0, f, 0] = taps(own_cells(fix, 0), in_ahead, in_behind) + taps(ghosts, cross_ahead, cross_behind)
            slope[1, f, 0] = own_rows_of(radial_of(fix_pad, f))
            slope[2, f, 0] = azimuthal
        dx, dr, da = ([slope[m, f, 0] for f in range(5)] for m in range(3))
        push = forcing(dx, dr, da)
        for f in range(5):
            change = -STEP_SIZE * (u[0] * dx[f] + u[1] * dr[f] + u[2] * da[f] + push[f])
            own_fix[f, 0, 0:16, :] = change
            if n == 0:
                for t in range(2):
                    rows = slice(8 * t, 8 * t + 8)
                    slots_a[1][2 + core, 5 * t + f] = next_pack[f, rows, :] + change[rows]
        return started

    result = (E.at[2, :, pl.ds(8, 8), pl.ds(row0, 16), :], out_hbm)
    started = step(0)
    started += step(1)

    def into_fix(f, carry):
        for t in range(2):
            for a in range(8):
                wide_fix[f, a, 8 * t:8 * t + 8, :] = widened(f, t, a)
        return carry

    lax.fori_loop(0, 5, into_fix, 0)
    store_fix = pltpu.make_async_copy(wide_fix, fix_hbm, local_sem.at[1])
    store_fix.start()
    for copy in started:
        copy.wait_send()
    pltpu.make_async_copy(*result, local_sem.at[0]).wait()
    store_fix.wait()


def shards(acoustic_state, mean_flow, sector_offset, cell_shift, stencil_start, interface_fraction):
    anywhere = pl.BlockSpec(memory_space=pl.ANY)
    vmem = lambda *shape: pltpu.VMEM(shape, F32)
    smem = lambda value: pltpu.SMEM(value.shape, value.dtype)
    without, ghosts = pl.pallas_call(
        kernel,
        out_shape=[jax.ShapeDtypeStruct(acoustic_state.shape, F32)] * 2,
        in_specs=[anywhere] * 6,
        out_specs=[anywhere] * 2,
        scratch_shapes=[
            smem(sector_offset),
            smem(cell_shift),
            smem(stencil_start),
            smem(interface_fraction),
            vmem(3, 5, 24, 40, 128),
            vmem(5, 16, 40, 128),
            *[vmem(count, 11, 8, 128) for count in (6, 3, NY, NX) for _ in range(2)],
            vmem(2, 3, 16, 8, 128),
            vmem(3, 2, 8, 128),
            vmem(3, 24, 128),
            vmem(3, 24, 128),
            vmem(5, 3, 16, 128),
            vmem(5, 2, 40, 128),
            vmem(3, 5, 2, 16, 128),
            vmem(5, 2, 16, 128),
            vmem(5, 2, 24, 128),
            vmem(5, 16, 128),
            vmem(5, 40, 128),
            vmem(5, 8, 16, 128),
            pltpu.SemaphoreType.DMA((2, 24)),
            pltpu.SemaphoreType.DMA((2, 24)),
            pltpu.SemaphoreType.DMA((3,)),
            pltpu.SemaphoreType.DMA((3,)),
            pltpu.SemaphoreType.DMA((6,)),
        ],
        compiler_params=pltpu.CompilerParams(collective_id=0, has_side_effects=True, vmem_limit_bytes=67043328),
        name="acoustic_steps",
    )(sector_offset, cell_shift, stencil_start, interface_fraction, mean_flow, acoustic_state)
    return without + ghosts


def solution(mesh):
    return jax.shard_map(
        shards,
        mesh=mesh,
        in_specs=(
            P(None, "azim", "rad", None),
            P(None, "rad", None),
            P(),
            P(None, "azim"),
            P(None, "azim"),
            P(None, "azim"),
        ),
        out_specs=P(None, "azim", "rad", None),
        check_vma=False,
    )
```

```python
import jax
import jax.numpy as jnp
from jax import lax
from jax.experimental import pallas as pl
from jax.experimental.pallas import tpu as pltpu
from jax.sharding import PartitionSpec as P

STENCIL = (0.841570125482, -0.244678631765, 0.059463584768, -0.007650904064)
STEP_SIZE = 0.2
MESH = pl.DeviceIdType.MESH
F32 = jnp.float32

NZ, NY, NX = 8, 4, 2
N = 128


def lanes(rows=8):
    return lax.broadcasted_iota(jnp.int32, (rows, 128), 1)


def moved(value, by):
    return value if by % 128 == 0 else pltpu.roll(value, (-by) % 128, value.ndim - 1)


def forcing(dx, dr, da):
    spread = dx[1] + dr[2] + da[3]
    return [spread, dx[4], dr[4], da[4], spread]


def kernel(offset_hbm, shift_hbm, start_hbm, fraction_hbm, flow_hbm, state_hbm, out_hbm, fix_hbm,
           offset_ref, shift_ref, start_ref, fraction_ref,
           E, mid, near_a0, near_a1, near_b0, near_b1, far_a0, far_a1, far_b0, far_b1, y_a0, y_a1, y_b0, y_b1, x_a0, x_a1, x_b0, x_b1, facing, own_coef, flow, flow_pack,
           own_pack, face_pad, slope, face_mid, own_fix, next_pack, fix_pad, wide_fix,
           send_sem, recv_sem, fixed_send, fixed_recv, local_sem):
    near_a, near_b, far_a, far_b = (near_a0, near_a1), (near_b0, near_b1), (far_a0, far_a1), (far_b0, far_b1)
    ys_a, ys_b, xs_a, xs_b = (y_a0, y_a1), (y_b0, y_b1), (x_a0, x_a1), (x_b0, x_b1)
    i = lax.axis_index("azim")
    r = lax.axis_index("rad")
    core, z, y, x = i % 2, (i // 2) % NZ, (i // 16) % NY, i // 64
    row0 = pl.multiple_of(8 + 8 * r, 8)
    far0 = pl.multiple_of(8 + 16 * r, 8)
    far0_here = pl.multiple_of(24 - 16 * r, 8)
    up, down = (i + 1) % N, (i + N - 1) % N

    def at(azim, rad=None):
        return {"azim": azim, "rad": r if rad is None else rad}

    def along_z(d):
        return i - 2 * z + 2 * ((z + d + NZ) % NZ)

    other = 1 - 2 * core
    near_to = [(i + other, 2 + core)]
    for d in (1, -1):
        near_to += [(along_z(d), 2 * (1 - d) + core), (along_z(d) + other, 2 * (1 - d) + core)]
    z_to = [(along_z(3), 0), (along_z(-3), 2)]
    y_to = [i - 16 * y + 16 * ((y + d) % NY) for d in (2, 1, 3)]
    x_to = (i + 64) % N

    loads = []

    def load(src, dst):
        copy = pltpu.make_async_copy(src, dst, local_sem.at[len(loads)])
        copy.start()
        loads.append(copy)

    load(state_hbm, E.at[0, :, pl.ds(8, 8), pl.ds(row0, 16), :])
    load(flow_hbm, flow.at[:, pl.ds(pl.multiple_of(8 * r, 8), 16), :])
    load(shift_hbm, shift_ref)
    load(start_hbm, start_ref)
    load(fraction_hbm, fraction_ref)
    load(offset_hbm, offset_ref)

    barrier = pltpu.get_barrier_semaphore()
    partners = [at(j) for j, _ in near_to] + [at(j) for j, _ in z_to] + [at(j) for j in y_to] + [at(x_to)]
    partners += [at(up), at(down), at(i, 1 - r), at(up, 1 - r), at(down, 1 - r)]
    for partner in partners:
        pl.semaphore_signal(barrier, inc=1, device_id=partner, device_id_type=MESH)

    edge = jnp.zeros((5, 16, 8, 128), F32)
    for n in range(2):
        E[n, :, 4:20, 0:8, :] = edge
        E[n, :, 4:20, 32:40, :] = edge
    for low in (0, 32):
        mid[:, :, low:low + 8, :] = edge
        face_pad[:, :, low:low + 8, :] = jnp.zeros((5, 2, 8, 128), F32)
        fix_pad[:, low:low + 8, :] = jnp.zeros((5, 8, 128), F32)

    lane = lanes()
    cell_of = (lane // 16 + 4) % 8
    upper = lane % 16 >= 8
    row = lax.broadcasted_iota(jnp.int32, (8, 128), 0)

    def spread_cells(get):
        value = jnp.full((8, 128), get(0))
        for a in range(1, 8):
            value = jnp.where(cell_of == a, get(a), value)
        return value

    def weights(t, m):
        up_one, down_one, down_two = t + 1.0, t - 1.0, t - 2.0
        w = (-t * down_one * down_two / 6.0, up_one * down_one * down_two / 2.0,
             -up_one * t * down_two / 2.0, up_one * t * down_one / 6.0)
        value = jnp.zeros((8, 128), F32)
        for p in range(4):
            value = jnp.where(m == p, w[p], value)
        return value

    def pack_rows(n, t, f):
        rows = pl.ds(pl.multiple_of(row0 + 8 * t, 8), 8)
        packed = None
        for a in range(8):
            turned = moved(E[n, f, 8 + a, rows, :], 56 - 16 * ((a + 4) % 8))
            packed = turned if packed is None else jnp.where(cell_of == a, turned, packed)
        return packed

    for copy in loads:
        copy.wait()
    for f in range(5):
        near_a[0][2 + core, f] = pack_rows(0, 0, f)
        ys_b[0][y, f] = pack_rows(0, 1, f)
    stator_t = spread_cells(lambda a: fraction_ref[0, a])
    rotor_t = spread_cells(lambda a: fraction_ref[1, a])
    for n in range(2):
        stator = weights(stator_t, row - spread_cells(lambda a: shift_ref[n, a] + start_ref[0, a] + 3))
        rotor = weights(rotor_t, row - spread_cells(lambda a: start_ref[1, a] - shift_ref[n, a]))
        own_coef[1, n] = jnp.where(upper, stator, rotor)
        near_a[n][2 + core, 5] = jnp.where(upper, rotor, stator)

    pl.semaphore_wait(barrier, len(partners))
    fixed = []

    def send_fixed(src, dst, to):
        no = len(fixed)
        copy = pltpu.make_async_remote_copy(src, dst, fixed_send.at[no], fixed_recv.at[no], device_id=to, device_id_type=MESH)
        copy.start()
        fixed.append(copy)

    half = lane % 64
    strip = lane % 16
    ahead = [jnp.where(half + j < 64, STENCIL[j - 1], 0.0) for j in range(1, 5)]
    behind = [jnp.where(half - j >= 0, STENCIL[j - 1], 0.0) for j in range(1, 5)]

    in_ahead = [jnp.where(strip % 8 + j < 8, STENCIL[j - 1], 0.0) for j in range(1, 5)]
    in_behind = [jnp.where(strip % 8 - j >= 0, STENCIL[j - 1], 0.0) for j in range(1, 5)]
    cross_ahead = [jnp.where((strip < 8) & (strip + j >= 8), STENCIL[j - 1], 0.0) for j in range(1, 5)]
    cross_behind = [jnp.where((strip >= 8) & (strip - j < 8), STENCIL[j - 1], 0.0) for j in range(1, 5)]

    def taps(value, fore, aft):
        total = None
        for j in range(1, 5):
            term = fore[j - 1][0:1] * moved(value, j) - aft[j - 1][0:1] * moved(value, -j)
            total = term if total is None else total + term
        return total

    def ring(sectors):
        low = lanes(sectors[0].shape[0]) < 64
        return [jnp.where(low, sectors[p], sectors[(p + 1) % 3]) for p in range(3)]

    def by_cells(packs, d):
        if d == 0:
            return packs[:2]
        at_lane = lanes(packs[0].shape[0])
        turned = [moved(v, 16 * d) for v in packs]
        if d > 0:
            return [jnp.where(at_lane < 128 - 16 * d, turned[p], turned[p + 1]) for p in range(2)]
        return [jnp.where(at_lane >= -16 * d, turned[p], turned[(p + 2) % 3]) for p in range(2)]

    def own_cells(packs, d):
        at_lane = lanes(packs[0].shape[0])
        first, last = (moved(v, 16 * d) for v in packs)
        if d >= 0:
            return jnp.where((at_lane >= 64) & (at_lane < 128 - 16 * d), first, last)
        return jnp.where((at_lane < 64) & (at_lane >= -16 * d), last, first)

    def evaluate_rows(ref, c, low):
        dx, dr, da, mine = [], [], [], []
        rows = pl.ds(low, 8)
        for f in range(5):
            here = ref[f, c, rows, :]
            mine.append(here)
            dx.append(taps(here, ahead, behind))
            radial = azimuthal = None
            for j in range(1, 5):
                step = STENCIL[j - 1] * (ref[f, c, pl.ds(low + j, 8), :] - ref[f, c, pl.ds(low - j, 8), :])
                radial = step if radial is None else radial + step
                step = STENCIL[j - 1] * (ref[f, c + j, rows, :] - ref[f, c - j, rows, :])
                azimuthal = step if azimuthal is None else azimuthal + step
            dr.append(radial)
            da.append(azimuthal)
        u = [flow[k, pl.ds(pl.multiple_of(low - 8, 8), 8), :] for k in range(3)]
        push = forcing(dx, dr, da)
        return mine, [-(u[0] * dx[f] + u[1] * dr[f] + u[2] * da[f]) - push[f] for f in range(5)]

    def radial_of(ref, *index):
        total = None
        for j in range(1, 5):
            part = STENCIL[j - 1] * (ref[(*index, slice(8 + j, 32 + j))] - ref[(*index, slice(8 - j, 32 - j))])
            total = part if total is None else total + part
        return total

    def own_rows_of(value):
        return jnp.where(r == 0, value[0:16], value[8:24])

    def widened(f, t, a):
        change = own_fix[f, 0, 8 * t:8 * t + 8, :]
        return jnp.where((lane >= 56) & (lane < 72), moved(change, 16 * ((a + 4) % 8) - 56), 0.0)

    def step(n):
        k = offset_ref[n]
        source_r = (i - k + N) % N
        source_s = (i + k) % N
        low_r = (core - k % 16 + 16) % 16
        low_s = (core + k % 16) % 16
        started = []

        def parts(low):
            far = ((low // 2 + 3) % 8 + 1) // 3 - 1
            near = (low // 2 + 3) % 8 - 3 - 3 * far
            return near, far

        def send(src, dst, to):
            no = len(started)
            copy = pltpu.make_async_remote_copy(src, dst, send_sem.at[n, no], recv_sem.at[n, no], device_id=to, device_id_type=MESH)
            copy.start()
            started.append(copy)
            return copy

        def chosen(slots, from_r, from_s):
            return jnp.where(upper[None], slots[from_r], slots[from_s])

        def along(slots, own, targets):
            mine = slots.at[own]
            return [send(mine, slots.at[place], at(j)) for j, place in targets]

        def arrived(copies):
            for copy in copies:
                copy.wait_recv()

        low = i % 16
        high = i // 16
        high_r = (high - k // 16 - (low + k % 16) // 16 + 16) % 8
        high_s = (high + k // 16 + (k % 16 + 15 - low) // 16) % 8
        (near_r, far_r), (near_s, far_s) = parts(low_r), parts(low_s)
        near_of = (2 * (near_r + 1) + low_r % 2, 2 * (near_s + 1) + low_s % 2)
        ys = [(j, y) for j in y_to]
        xs = [(x_to, x)]

        stage_a = along(near_a[n], 2 + core, near_to)
        stage_b = along(ys_b[n], y, ys)

        if n == 0:
            send_fixed(own_coef.at[1], own_coef.at[0], at(up))
            send_fixed(own_coef.at[1], own_coef.at[2], at(down))
            send_fixed(flow.at[:, pl.ds(8, 8), :], flow.at[:, pl.ds(pl.multiple_of(16 * r, 8), 8), :], at(i, 1 - r))
        else:
            def into_rows(f, carry):
                for t in range(2):
                    rows = pl.ds(pl.multiple_of(row0 + 8 * t, 8), 8)
                    for a in range(8):
                        E[1, f, 8 + a, rows, :] = E[1, f, 8 + a, rows, :] + widened(f, t, a)
                return carry

            lax.fori_loop(0, 5, into_rows, 0)

        own_rows, far_rows = pl.ds(row0, 16), pl.ds(far0, 8)
        halos = []

        def halo_cells(fields):
            part = E.at[n, fields, pl.ds(8, 8), own_rows, :]
            halos.append(send(part, E.at[n, fields, pl.ds(0, 8), own_rows, :], at(up)))
            halos.append(send(part, E.at[n, fields, pl.ds(16, 8), own_rows, :], at(down)))

        halos.append(send(E.at[n, :, pl.ds(8, 8), pl.ds(16, 8), :], E.at[n, :, pl.ds(8, 8), far_rows, :], at(i, 1 - r)))
        halo_cells(pl.ds(0, 2))
        arrived(stage_a)
        far_a[n][1] = chosen(near_a[n], *near_of)
        stage_a = along(far_a[n], 1, z_to)
        arrived(stage_b)
        xs_b[n][x] = chosen(ys_b[n], high_r % NY, high_s % NY)
        stage_b = along(xs_b[n], x, xs)
        halo_cells(pl.ds(2, 1))

        arrived(stage_b)
        near_b[n][2 + core] = chosen(xs_b[n], high_r // NY, high_s // NY)
        stage_b = along(near_b[n], 2 + core, near_to)
        halos.append(send(E.at[n, :, pl.ds(12, 4), pl.ds(16, 8), :], E.at[n, :, pl.ds(4, 4), far_rows, :], at(up, 1 - r)))
        halos.append(send(E.at[n, :, pl.ds(8, 4), pl.ds(16, 8), :], E.at[n, :, pl.ds(16, 4), far_rows, :], at(down, 1 - r)))
        arrived(stage_a)
        ys_a[n][y] = chosen(far_a[n], far_r + 1, far_s + 1)
        stage_a = along(ys_a[n], y, ys)
        halo_cells(pl.ds(3, 2))

        arrived(stage_b)
        far_b[n][1] = chosen(near_b[n], *near_of)
        stage_b = along(far_b[n], 1, z_to)
        arrived(stage_a)
        xs_a[n][x] = chosen(ys_a[n], (source_r // 16) % NY, (source_s // 16) % NY)
        stage_a = along(xs_a[n], x, xs)

        if n == 0:
            for copy in fixed:
                copy.wait()
            for m in range(3):
                packed = None
                for a in range(8):
                    turned = moved(flow[m], 56 - 16 * a)
                    packed = turned if packed is None else jnp.where(lanes(24) // 16 == a, turned, packed)
                flow_pack[m] = packed
        for copy in halos:
            copy.wait_recv()

        def midpoint(c, low):
            here, slopes = evaluate_rows(E.at[n], c + 4, low)
            for f in range(5):
                mid[f, c, pl.ds(low, 8), :] = here[f] + (0.5 * STEP_SIZE) * slopes[f]

        def first(c, carry):
            midpoint(c, row0)
            midpoint(c, pl.multiple_of(row0 + 8, 8))
            return carry

        def first_far(c, carry):
            midpoint(c + 4, far0_here)
            return carry

        lax.fori_loop(0, 16, first, 0)
        lax.fori_loop(0, 8, first_far, 0)
        arrived(stage_a)
        got = chosen(xs_a[n], source_r // 64, source_s // 64)
        facing[n, 1, pl.ds(5 * r, 5)] = got[0:5]
        facing[n, 1, 15] = got[5]
        arrived(stage_b)
        facing[n, 1, pl.ds(5 * r + 5, 5)] = chosen(far_b[n], far_r + 1, far_s + 1)
        rows10, rows5 = pl.ds(5 * r, 10), pl.ds(10 * r, 5)
        stage = []
        for to, place in ((up, 0), (down, 2)):
            stage.append(send(facing.at[n, 1, rows10], facing.at[n, place, rows10], at(to)))
            stage.append(send(facing.at[n, 1, 15], facing.at[n, place, 15], at(to)))
            stage.append(send(facing.at[n, 1, pl.ds(5, 5)], facing.at[n, place, rows5], at(to, 1 - r)))
        stage.append(send(facing.at[n, 1, pl.ds(5, 5)], facing.at[n, 1, rows5], at(i, 1 - r)))

        def second(c, carry):
            for t in range(2):
                low = pl.multiple_of(row0 + 8 * t, 8)
                _, slopes = evaluate_rows(mid, c + 4, low)
                for f in range(5):
                    E[n + 1, f, c + 8, pl.ds(low, 8), :] = E[n, f, c + 8, pl.ds(low, 8), :] + STEP_SIZE * slopes[f]
            return carry

        lax.fori_loop(0, 8, second, 0)
        if n == 1:
            pltpu.make_async_copy(*result, local_sem.at[0]).start()

        def strip_of(f, carry):
            for p in range(3):
                packed = None
                for a in range(8):
                    turned = moved(E[n, f, (4 + 8 * p + a) % 24, own_rows, :], 56 - 16 * a)
                    packed = turned if packed is None else jnp.where(lanes(16) // 16 == a, turned, packed)
                own_pack[f, p] = packed
            if n == 0:
                for t in range(2):
                    next_pack[f, 8 * t:8 * t + 8, :] = pack_rows(1, t, f)
            return carry

        lax.fori_loop(0, 5, strip_of, 0)
        coef_own = ring([own_coef[p, n] for p in range(3)])
        u24 = [flow_pack[m] for m in range(3)]
        u = [flow_pack[m, pl.ds(pl.multiple_of(8 * r, 8), 16), :] for m in range(3)]
        for copy in stage:
            copy.wait_recv()

        coef_face = ring([jnp.where(upper, moved(facing[n, p, 15], -8), moved(facing[n, p, 15], 8)) for p in range(3)])

        for f in range(5):
            F = ring([jnp.concatenate([facing[n, p, 5 * t + f] for t in range(3)], axis=0) for p in range(3)])
            M = [own_pack[f, p] for p in range(3)]
            F_own = [own_rows_of(v) for v in F]
            for p in range(2):
                face_pad[f, p, 8:32, :] = F[p]
            ghost_own = [jnp.zeros((24, 128), F32)] * 2
            ghost_face = [jnp.zeros((16, 128), F32)] * 2
            azimuthal = [jnp.zeros((16, 128), F32)] * 2
            for d in range(-4, 5):
                shifted = by_cells(F if d < 4 else F_own, d)
                if d < 4:
                    shifted_own = by_cells(M, d)
                for p in range(2):
                    if d != 0:
                        weight = STENCIL[d - 1] if d > 0 else -STENCIL[-d - 1]
                        azimuthal[p] = azimuthal[p] + weight * (own_rows_of(shifted[p]) if d < 4 else shifted[p])
                    if d < 4:
                        ghost_own[p] = ghost_own[p] + coef_own[p][d + 4:d + 5, :] * shifted[p]
                        ghost_face[p] = ghost_face[p] + coef_face[p][d + 4:d + 5, :] * shifted_own[p]
            for p in range(2):
                slope[0, f, p] = taps(F_own[p], in_ahead, in_behind) + taps(ghost_face[p], cross_ahead, cross_behind)
                slope[1, f, p] = own_rows_of(radial_of(face_pad, f, p))
                slope[2, f, p] = azimuthal[p]
                own_fix[f, p] = taps(ghost_own[p], cross_ahead, cross_behind)

        for p in range(2):
            dx, dr, da = ([slope[m, f, p] for f in range(5)] for m in range(3))
            push = forcing(dx, dr, da)
            for f in range(5):
                change = -(u[0] * dx[f] + u[1] * dr[f] + u[2] * da[f]) - push[f]
                face_mid[f, p] = face_pad[f, p, own_rows, :] + (0.5 * STEP_SIZE) * change
            cut = [own_fix[f, p] for f in range(5)]
            push = [cut[1], cut[4], 0.0, 0.0, cut[1]]
            for f in range(5):
                own_fix[f, p] = (-0.5 * STEP_SIZE) * (u24[0] * cut[f] + push[f])

        for f in range(5):
            face = [face_mid[f, p] for p in range(2)]
            fix = [own_rows_of(own_fix[f, p]) for p in range(2)]
            fix_pad[f, 8:32, :] = own_cells([own_fix[f, p] for p in range(2)], 0)
            ghosts = jnp.zeros((16, 128), F32)
            azimuthal = jnp.zeros((16, 128), F32)
            for d in range(-4, 5):
                if d < 4:
                    ghosts = ghosts + own_coef[1, n, d + 4:d + 5, :] * own_cells(face, d)
                if d != 0:
                    weight = STENCIL[d - 1] if d > 0 else -STENCIL[-d - 1]
                    azimuthal = azimuthal + weight * own_cells(fix, d)
            slope[0, f, 0] = taps(own_cells(fix, 0), in_ahead, in_behind) + taps(ghosts, cross_ahead, cross_behind)
            slope[1, f, 0] = own_rows_of(radial_of(fix_pad, f))
            slope[2, f, 0] = azimuthal
        dx, dr, da = ([slope[m, f, 0] for f in range(5)] for m in range(3))
        push = forcing(dx, dr, da)
        for f in range(5):
            change = -STEP_SIZE * (u[0] * dx[f] + u[1] * dr[f] + u[2] * da[f] + push[f])
            own_fix[f, 0, 0:16, :] = change
            if n == 0:
                after = next_pack[f] + change
                near_a[1][2 + core, f] = after[0:8]
                ys_b[1][y, f] = after[8:16]
        return started

    result = (E.at[2, :, pl.ds(8, 8), pl.ds(row0, 16), :], out_hbm)
    started = step(0)
    started += step(1)

    def into_fix(f, carry):
        for t in range(2):
            for a in range(8):
                wide_fix[f, a, 8 * t:8 * t + 8, :] = widened(f, t, a)
        return carry

    lax.fori_loop(0, 5, into_fix, 0)
    store_fix = pltpu.make_async_copy(wide_fix, fix_hbm, local_sem.at[1])
    store_fix.start()
    for copy in started:
        copy.wait_send()
    pltpu.make_async_copy(*result, local_sem.at[0]).wait()
    store_fix.wait()


def shards(acoustic_state, mean_flow, sector_offset, cell_shift, stencil_start, interface_fraction):
    anywhere = pl.BlockSpec(memory_space=pl.ANY)
    vmem = lambda *shape: pltpu.VMEM(shape, F32)
    smem = lambda value: pltpu.SMEM(value.shape, value.dtype)
    without, ghosts = pl.pallas_call(
        kernel,
        out_shape=[jax.ShapeDtypeStruct(acoustic_state.shape, F32)] * 2,
        in_specs=[anywhere] * 6,
        out_specs=[anywhere] * 2,
        scratch_shapes=[
            smem(sector_offset),
            smem(cell_shift),
            smem(stencil_start),
            smem(interface_fraction),
            vmem(3, 5, 24, 40, 128),
            vmem(5, 16, 40, 128),
            *[vmem(count, tiles, 8, 128) for count in (6, 3, NY, NX) for tiles in (6, 5) for _ in range(2)],
            vmem(2, 3, 16, 8, 128),
            vmem(3, 2, 8, 128),
            vmem(3, 24, 128),
            vmem(3, 24, 128),
            vmem(5, 3, 16, 128),
            vmem(5, 2, 40, 128),
            vmem(3, 5, 2, 16, 128),
            vmem(5, 2, 16, 128),
            vmem(5, 2, 24, 128),
            vmem(5, 16, 128),
            vmem(5, 40, 128),
            vmem(5, 8, 16, 128),
            pltpu.SemaphoreType.DMA((2, 40)),
            pltpu.SemaphoreType.DMA((2, 40)),
            pltpu.SemaphoreType.DMA((3,)),
            pltpu.SemaphoreType.DMA((3,)),
            pltpu.SemaphoreType.DMA((6,)),
        ],
        compiler_params=pltpu.CompilerParams(collective_id=0, has_side_effects=True, vmem_limit_bytes=67043328),
        name="acoustic_steps",
    )(sector_offset, cell_shift, stencil_start, interface_fraction, mean_flow, acoustic_state)
    return without + ghosts


def solution(mesh):
    return jax.shard_map(
        shards,
        mesh=mesh,
        in_specs=(
            P(None, "azim", "rad", None),
            P(None, "rad", None),
            P(),
            P(None, "azim"),
            P(None, "azim"),
            P(None, "azim"),
        ),
        out_specs=P(None, "azim", "rad", None),
        check_vma=False,
    )
```

```python
import jax
import jax.numpy as jnp
from jax import lax
from jax.experimental import pallas as pl
from jax.experimental.pallas import tpu as pltpu
from jax.sharding import PartitionSpec as P

STENCIL = (0.841570125482, -0.244678631765, 0.059463584768, -0.007650904064)
STEP_SIZE = 0.2
MESH = pl.DeviceIdType.MESH
F32 = jnp.float32

NZ, NY, NX = 8, 4, 2
N = 128


def lanes(rows=8):
    return lax.broadcasted_iota(jnp.int32, (rows, 128), 1)


def moved(value, by):
    return value if by % 128 == 0 else pltpu.roll(value, (-by) % 128, value.ndim - 1)


def forcing(dx, dr, da):
    spread = dx[1] + dr[2] + da[3]
    return [spread, dx[4], dr[4], da[4], spread]


def kernel(offset_hbm, shift_hbm, start_hbm, fraction_hbm, flow_hbm, state_hbm, out_hbm, fix_hbm,
           offset_ref, shift_ref, start_ref, fraction_ref,
           E, mid, near_a0, near_a1, near_b0, near_b1, far_a0, far_a1, far_b0, far_b1, y_a0, y_a1, y_b0, y_b1, x_a0, x_a1, x_b0, x_b1, facing, own_coef, flow, flow_pack,
           own_pack, face_pad, slope, face_mid, own_fix, next_pack, fix_pad, wide_fix,
           send_sem, recv_sem, fixed_send, fixed_recv, local_sem):
    near_a, near_b, far_a, far_b = (near_a0, near_a1), (near_b0, near_b1), (far_a0, far_a1), (far_b0, far_b1)
    ys_a, ys_b, xs_a, xs_b = (y_a0, y_a1), (y_b0, y_b1), (x_a0, x_a1), (x_b0, x_b1)
    i = lax.axis_index("azim")
    r = lax.axis_index("rad")
    core, z, y, x = i % 2, (i // 2) % NZ, (i // 16) % NY, i // 64
    row0 = pl.multiple_of(8 + 8 * r, 8)
    far0 = pl.multiple_of(8 + 16 * r, 8)
    far0_here = pl.multiple_of(24 - 16 * r, 8)
    up, down = (i + 1) % N, (i + N - 1) % N

    def at(azim, rad=None):
        return {"azim": azim, "rad": r if rad is None else rad}

    def along_z(d):
        return i - 2 * z + 2 * ((z + d + NZ) % NZ)

    other = 1 - 2 * core
    near_to = [(i + other, 2 + core)]
    for d in (1, -1):
        near_to += [(along_z(d), 2 * (1 - d) + core), (along_z(d) + other, 2 * (1 - d) + core)]
    z_to = [(along_z(3), 0), (along_z(-3), 2)]
    y_to = [i - 16 * y + 16 * ((y + d) % NY) for d in (2, 1, 3)]
    x_to = (i + 64) % N

    loads = []

    def load(src, dst):
        copy = pltpu.make_async_copy(src, dst, local_sem.at[len(loads)])
        copy.start()
        loads.append(copy)

    load(state_hbm, E.at[0, :, pl.ds(8, 8), pl.ds(row0, 16), :])
    load(flow_hbm, flow.at[:, pl.ds(pl.multiple_of(8 * r, 8), 16), :])
    load(shift_hbm, shift_ref)
    load(start_hbm, start_ref)
    load(fraction_hbm, fraction_ref)
    load(offset_hbm, offset_ref)

    barrier = pltpu.get_barrier_semaphore()
    partners = [at(j) for j, _ in near_to] + [at(j) for j, _ in z_to] + [at(j) for j in y_to] + [at(x_to)]
    partners += [at(up), at(down), at(i, 1 - r), at(up, 1 - r), at(down, 1 - r)]
    for partner in partners:
        pl.semaphore_signal(barrier, inc=1, device_id=partner, device_id_type=MESH)

    edge = jnp.zeros((5, 16, 8, 128), F32)
    for n in range(2):
        E[n, :, 4:20, 0:8, :] = edge
        E[n, :, 4:20, 32:40, :] = edge
    for low in (0, 32):
        mid[:, :, low:low + 8, :] = edge
        face_pad[:, :, low:low + 8, :] = jnp.zeros((5, 2, 8, 128), F32)
        fix_pad[:, low:low + 8, :] = jnp.zeros((5, 8, 128), F32)

    lane = lanes()
    cell_of = (lane // 16 + 4) % 8
    upper = lane % 16 >= 8
    row = lax.broadcasted_iota(jnp.int32, (8, 128), 0)

    def spread_cells(get):
        value = jnp.full((8, 128), get(0))
        for a in range(1, 8):
            value = jnp.where(cell_of == a, get(a), value)
        return value

    def weights(t, m):
        up_one, down_one, down_two = t + 1.0, t - 1.0, t - 2.0
        w = (-t * down_one * down_two / 6.0, up_one * down_one * down_two / 2.0,
             -up_one * t * down_two / 2.0, up_one * t * down_one / 6.0)
        value = jnp.zeros((8, 128), F32)
        for p in range(4):
            value = jnp.where(m == p, w[p], value)
        return value

    def pack_rows(n, t, f):
        rows = pl.ds(pl.multiple_of(row0 + 8 * t, 8), 8)
        packed = None
        for a in range(8):
            turned = moved(E[n, f, 8 + a, rows, :], 56 - 16 * ((a + 4) % 8))
            packed = turned if packed is None else jnp.where(cell_of == a, turned, packed)
        return packed

    for copy in loads:
        copy.wait()
    for f in range(5):
        near_a[0][2 + core, f] = pack_rows(0, 0, f)
        ys_b[0][y, f] = pack_rows(0, 1, f)
    stator_t = spread_cells(lambda a: fraction_ref[0, a])
    rotor_t = spread_cells(lambda a: fraction_ref[1, a])
    for n in range(2):
        stator = weights(stator_t, row - spread_cells(lambda a: shift_ref[n, a] + start_ref[0, a] + 3))
        rotor = weights(rotor_t, row - spread_cells(lambda a: start_ref[1, a] - shift_ref[n, a]))
        own_coef[1, n] = jnp.where(upper, stator, rotor)
        near_a[n][2 + core, 5] = jnp.where(upper, rotor, stator)

    pl.semaphore_wait(barrier, len(partners))
    fixed = []

    def send_fixed(src, dst, to):
        no = len(fixed)
        copy = pltpu.make_async_remote_copy(src, dst, fixed_send.at[no], fixed_recv.at[no], device_id=to, device_id_type=MESH)
        copy.start()
        fixed.append(copy)

    half = lane % 64
    strip = lane % 16
    ahead = [jnp.where(half + j < 64, STENCIL[j - 1], 0.0) for j in range(1, 5)]
    behind = [jnp.where(half - j >= 0, STENCIL[j - 1], 0.0) for j in range(1, 5)]

    in_ahead = [jnp.where(strip % 8 + j < 8, STENCIL[j - 1], 0.0) for j in range(1, 5)]
    in_behind = [jnp.where(strip % 8 - j >= 0, STENCIL[j - 1], 0.0) for j in range(1, 5)]
    cross_ahead = [jnp.where((strip < 8) & (strip + j >= 8), STENCIL[j - 1], 0.0) for j in range(1, 5)]
    cross_behind = [jnp.where((strip >= 8) & (strip - j < 8), STENCIL[j - 1], 0.0) for j in range(1, 5)]

    def taps(value, fore, aft):
        total = None
        for j in range(1, 5):
            term = fore[j - 1][0:1] * moved(value, j) - aft[j - 1][0:1] * moved(value, -j)
            total = term if total is None else total + term
        return total

    def ring(sectors):
        low = lanes(sectors[0].shape[0]) < 64
        return [jnp.where(low, sectors[p], sectors[(p + 1) % 3]) for p in range(3)]

    def by_cells(packs, d):
        if d == 0:
            return packs[:2]
        at_lane = lanes(packs[0].shape[0])
        turned = [moved(v, 16 * d) for v in packs]
        if d > 0:
            return [jnp.where(at_lane < 128 - 16 * d, turned[p], turned[p + 1]) for p in range(2)]
        return [jnp.where(at_lane >= -16 * d, turned[p], turned[(p + 2) % 3]) for p in range(2)]

    def own_cells(packs, d):
        at_lane = lanes(packs[0].shape[0])
        first, last = (moved(v, 16 * d) for v in packs)
        if d >= 0:
            return jnp.where((at_lane >= 64) & (at_lane < 128 - 16 * d), first, last)
        return jnp.where((at_lane < 64) & (at_lane >= -16 * d), last, first)

    def evaluate_rows(ref, c, low):
        dx, dr, da, mine = [], [], [], []
        rows = pl.ds(low, 8)
        for f in range(5):
            here = ref[f, c, rows, :]
            mine.append(here)
            dx.append(taps(here, ahead, behind))
            radial = azimuthal = None
            for j in range(1, 5):
                step = STENCIL[j - 1] * (ref[f, c, pl.ds(low + j, 8), :] - ref[f, c, pl.ds(low - j, 8), :])
                radial = step if radial is None else radial + step
                step = STENCIL[j - 1] * (ref[f, c + j, rows, :] - ref[f, c - j, rows, :])
                azimuthal = step if azimuthal is None else azimuthal + step
            dr.append(radial)
            da.append(azimuthal)
        u = [flow[k, pl.ds(pl.multiple_of(low - 8, 8), 8), :] for k in range(3)]
        push = forcing(dx, dr, da)
        return mine, [-(u[0] * dx[f] + u[1] * dr[f] + u[2] * da[f]) - push[f] for f in range(5)]

    def radial_of(ref, *index):
        total = None
        for j in range(1, 5):
            part = STENCIL[j - 1] * (ref[(*index, slice(8 + j, 32 + j))] - ref[(*index, slice(8 - j, 32 - j))])
            total = part if total is None else total + part
        return total

    def own_rows_of(value):
        return jnp.where(r == 0, value[0:16], value[8:24])

    def widened(f, t, a):
        change = own_fix[f, 0, 8 * t:8 * t + 8, :]
        return jnp.where((lane >= 56) & (lane < 72), moved(change, 16 * ((a + 4) % 8) - 56), 0.0)

    def step(n):
        k = offset_ref[n]
        source_r = (i - k + N) % N
        source_s = (i + k) % N
        low_r = (core - k % 16 + 16) % 16
        low_s = (core + k % 16) % 16
        started = []

        def parts(low):
            far = ((low // 2 + 3) % 8 + 1) // 3 - 1
            near = (low // 2 + 3) % 8 - 3 - 3 * far
            return near, far

        def send(src, dst, to):
            no = len(started)
            copy = pltpu.make_async_remote_copy(src, dst, send_sem.at[n, no], recv_sem.at[n, no], device_id=to, device_id_type=MESH)
            copy.start()
            started.append(copy)
            return copy

        def chosen(slots, from_r, from_s):
            return jnp.where(upper[None], slots[from_r], slots[from_s])

        def along(slots, own, targets):
            mine = slots.at[own]
            return [send(mine, slots.at[place], at(j)) for j, place in targets]

        def arrived(copies):
            for copy in copies:
                copy.wait_recv()

        low = i % 16
        high = i // 16
        high_r = (high - k // 16 - (low + k % 16) // 16 + 16) % 8
        high_s = (high + k // 16 + (k % 16 + 15 - low) // 16) % 8
        (near_r, far_r), (near_s, far_s) = parts(low_r), parts(low_s)
        near_of = (2 * (near_r + 1) + low_r % 2, 2 * (near_s + 1) + low_s % 2)
        ys = [(j, y) for j in y_to]
        xs = [(x_to, x)]

        stage_a = along(near_a[n], 2 + core, near_to)
        stage_b = along(ys_b[n], y, ys)

        if n == 0:
            send_fixed(own_coef.at[1], own_coef.at[0], at(up))
            send_fixed(own_coef.at[1], own_coef.at[2], at(down))
            send_fixed(flow.at[:, pl.ds(8, 8), :], flow.at[:, pl.ds(pl.multiple_of(16 * r, 8), 8), :], at(i, 1 - r))
        else:
            def into_rows(f, carry):
                for t in range(2):
                    rows = pl.ds(pl.multiple_of(row0 + 8 * t, 8), 8)
                    for a in range(8):
                        E[1, f, 8 + a, rows, :] = E[1, f, 8 + a, rows, :] + widened(f, t, a)
                return carry

            lax.fori_loop(0, 5, into_rows, 0)

        own_rows, far_rows = pl.ds(row0, 16), pl.ds(far0, 8)
        halos = []

        def halo_cells(fields):
            part = E.at[n, fields, pl.ds(8, 8), own_rows, :]
            halos.append(send(part, E.at[n, fields, pl.ds(0, 8), own_rows, :], at(up)))
            halos.append(send(part, E.at[n, fields, pl.ds(16, 8), own_rows, :], at(down)))

        halos.append(send(E.at[n, :, pl.ds(8, 8), pl.ds(16, 8), :], E.at[n, :, pl.ds(8, 8), far_rows, :], at(i, 1 - r)))
        halo_cells(pl.ds(0, 2))
        arrived(stage_a)
        far_a[n][1] = chosen(near_a[n], *near_of)
        stage_a = along(far_a[n], 1, z_to)
        arrived(stage_b)
        xs_b[n][x] = chosen(ys_b[n], high_r % NY, high_s % NY)
        stage_b = along(xs_b[n], x, xs)
        halo_cells(pl.ds(2, 1))

        arrived(stage_b)
        near_b[n][2 + core] = chosen(xs_b[n], high_r // NY, high_s // NY)
        stage_b = along(near_b[n], 2 + core, near_to)
        halos.append(send(E.at[n, :, pl.ds(12, 4), pl.ds(16, 8), :], E.at[n, :, pl.ds(4, 4), far_rows, :], at(up, 1 - r)))
        halos.append(send(E.at[n, :, pl.ds(8, 4), pl.ds(16, 8), :], E.at[n, :, pl.ds(16, 4), far_rows, :], at(down, 1 - r)))
        arrived(stage_a)
        ys_a[n][y] = chosen(far_a[n], far_r + 1, far_s + 1)
        stage_a = along(ys_a[n], y, ys)
        halo_cells(pl.ds(3, 2))

        arrived(stage_b)
        far_b[n][1] = chosen(near_b[n], *near_of)
        stage_b = along(far_b[n], 1, z_to)
        arrived(stage_a)
        xs_a[n][x] = chosen(ys_a[n], (source_r // 16) % NY, (source_s // 16) % NY)
        stage_a = along(xs_a[n], x, xs)

        if n == 0:
            for copy in fixed:
                copy.wait()
            for m in range(3):
                packed = None
                for a in range(8):
                    turned = moved(flow[m], 56 - 16 * a)
                    packed = turned if packed is None else jnp.where(lanes(24) // 16 == a, turned, packed)
                flow_pack[m] = packed
        arrived(stage_a)
        got = chosen(xs_a[n], source_r // 64, source_s // 64)
        facing[n, 1, pl.ds(5 * r, 5)] = got[0:5]
        facing[n, 1, 15] = got[5]
        arrived(stage_b)
        facing[n, 1, pl.ds(5 * r + 5, 5)] = chosen(far_b[n], far_r + 1, far_s + 1)
        rows10, rows5 = pl.ds(5 * r, 10), pl.ds(10 * r, 5)
        stage = []
        for to, place in ((up, 0), (down, 2)):
            stage.append(send(facing.at[n, 1, rows10], facing.at[n, place, rows10], at(to)))
            stage.append(send(facing.at[n, 1, 15], facing.at[n, place, 15], at(to)))
            stage.append(send(facing.at[n, 1, pl.ds(5, 5)], facing.at[n, place, rows5], at(to, 1 - r)))
        stage.append(send(facing.at[n, 1, pl.ds(5, 5)], facing.at[n, 1, rows5], at(i, 1 - r)))

        for copy in halos:
            copy.wait_recv()

        def midpoint(c, low):
            here, slopes = evaluate_rows(E.at[n], c + 4, low)
            for f in range(5):
                mid[f, c, pl.ds(low, 8), :] = here[f] + (0.5 * STEP_SIZE) * slopes[f]

        def first(c, carry):
            midpoint(c, row0)
            midpoint(c, pl.multiple_of(row0 + 8, 8))
            return carry

        def first_far(c, carry):
            midpoint(c + 4, far0_here)
            return carry

        lax.fori_loop(0, 16, first, 0)
        lax.fori_loop(0, 8, first_far, 0)
        def second(c, carry):
            for t in range(2):
                low = pl.multiple_of(row0 + 8 * t, 8)
                _, slopes = evaluate_rows(mid, c + 4, low)
                for f in range(5):
                    E[n + 1, f, c + 8, pl.ds(low, 8), :] = E[n, f, c + 8, pl.ds(low, 8), :] + STEP_SIZE * slopes[f]
            return carry

        lax.fori_loop(0, 8, second, 0)
        if n == 1:
            pltpu.make_async_copy(*result, local_sem.at[0]).start()

        def strip_of(f, carry):
            for p in range(3):
                packed = None
                for a in range(8):
                    turned = moved(E[n, f, (4 + 8 * p + a) % 24, own_rows, :], 56 - 16 * a)
                    packed = turned if packed is None else jnp.where(lanes(16) // 16 == a, turned, packed)
                own_pack[f, p] = packed
            if n == 0:
                for t in range(2):
                    next_pack[f, 8 * t:8 * t + 8, :] = pack_rows(1, t, f)
            return carry

        lax.fori_loop(0, 5, strip_of, 0)
        coef_own = ring([own_coef[p, n] for p in range(3)])
        u24 = [flow_pack[m] for m in range(3)]
        u = [flow_pack[m, pl.ds(pl.multiple_of(8 * r, 8), 16), :] for m in range(3)]
        for copy in stage:
            copy.wait_recv()

        coef_face = ring([jnp.where(upper, moved(facing[n, p, 15], -8), moved(facing[n, p, 15], 8)) for p in range(3)])

        for f in range(5):
            F = ring([jnp.concatenate([facing[n, p, 5 * t + f] for t in range(3)], axis=0) for p in range(3)])
            M = [own_pack[f, p] for p in range(3)]
            F_own = [own_rows_of(v) for v in F]
            for p in range(2):
                face_pad[f, p, 8:32, :] = F[p]
            ghost_own = [jnp.zeros((24, 128), F32)] * 2
            ghost_face = [jnp.zeros((16, 128), F32)] * 2
            azimuthal = [jnp.zeros((16, 128), F32)] * 2
            for d in range(-4, 5):
                shifted = by_cells(F if d < 4 else F_own, d)
                if d < 4:
                    shifted_own = by_cells(M, d)
                for p in range(2):
                    if d != 0:
                        weight = STENCIL[d - 1] if d > 0 else -STENCIL[-d - 1]
                        azimuthal[p] = azimuthal[p] + weight * (own_rows_of(shifted[p]) if d < 4 else shifted[p])
                    if d < 4:
                        ghost_own[p] = ghost_own[p] + coef_own[p][d + 4:d + 5, :] * shifted[p]
                        ghost_face[p] = ghost_face[p] + coef_face[p][d + 4:d + 5, :] * shifted_own[p]
            for p in range(2):
                slope[0, f, p] = taps(F_own[p], in_ahead, in_behind) + taps(ghost_face[p], cross_ahead, cross_behind)
                slope[1, f, p] = own_rows_of(radial_of(face_pad, f, p))
                slope[2, f, p] = azimuthal[p]
                own_fix[f, p] = taps(ghost_own[p], cross_ahead, cross_behind)

        for p in range(2):
            dx, dr, da = ([slope[m, f, p] for f in range(5)] for m in range(3))
            push = forcing(dx, dr, da)
            for f in range(5):
                change = -(u[0] * dx[f] + u[1] * dr[f] + u[2] * da[f]) - push[f]
                face_mid[f, p] = face_pad[f, p, own_rows, :] + (0.5 * STEP_SIZE) * change
            cut = [own_fix[f, p] for f in range(5)]
            push = [cut[1], cut[4], 0.0, 0.0, cut[1]]
            for f in range(5):
                own_fix[f, p] = (-0.5 * STEP_SIZE) * (u24[0] * cut[f] + push[f])

        for f in range(5):
            face = [face_mid[f, p] for p in range(2)]
            fix = [own_rows_of(own_fix[f, p]) for p in range(2)]
            fix_pad[f, 8:32, :] = own_cells([own_fix[f, p] for p in range(2)], 0)
            ghosts = jnp.zeros((16, 128), F32)
            azimuthal = jnp.zeros((16, 128), F32)
            for d in range(-4, 5):
                if d < 4:
                    ghosts = ghosts + own_coef[1, n, d + 4:d + 5, :] * own_cells(face, d)
                if d != 0:
                    weight = STENCIL[d - 1] if d > 0 else -STENCIL[-d - 1]
                    azimuthal = azimuthal + weight * own_cells(fix, d)
            slope[0, f, 0] = taps(own_cells(fix, 0), in_ahead, in_behind) + taps(ghosts, cross_ahead, cross_behind)
            slope[1, f, 0] = own_rows_of(radial_of(fix_pad, f))
            slope[2, f, 0] = azimuthal
        dx, dr, da = ([slope[m, f, 0] for f in range(5)] for m in range(3))
        push = forcing(dx, dr, da)
        for f in range(5):
            change = -STEP_SIZE * (u[0] * dx[f] + u[1] * dr[f] + u[2] * da[f] + push[f])
            own_fix[f, 0, 0:16, :] = change
            if n == 0:
                after = next_pack[f] + change
                near_a[1][2 + core, f] = after[0:8]
                ys_b[1][y, f] = after[8:16]
        return started

    result = (E.at[2, :, pl.ds(8, 8), pl.ds(row0, 16), :], out_hbm)
    started = step(0)
    started += step(1)

    def into_fix(f, carry):
        for t in range(2):
            for a in range(8):
                wide_fix[f, a, 8 * t:8 * t + 8, :] = widened(f, t, a)
        return carry

    lax.fori_loop(0, 5, into_fix, 0)
    store_fix = pltpu.make_async_copy(wide_fix, fix_hbm, local_sem.at[1])
    store_fix.start()
    for copy in started:
        copy.wait_send()
    pltpu.make_async_copy(*result, local_sem.at[0]).wait()
    store_fix.wait()


def shards(acoustic_state, mean_flow, sector_offset, cell_shift, stencil_start, interface_fraction):
    anywhere = pl.BlockSpec(memory_space=pl.ANY)
    vmem = lambda *shape: pltpu.VMEM(shape, F32)
    smem = lambda value: pltpu.SMEM(value.shape, value.dtype)
    without, ghosts = pl.pallas_call(
        kernel,
        out_shape=[jax.ShapeDtypeStruct(acoustic_state.shape, F32)] * 2,
        in_specs=[anywhere] * 6,
        out_specs=[anywhere] * 2,
        scratch_shapes=[
            smem(sector_offset),
            smem(cell_shift),
            smem(stencil_start),
            smem(interface_fraction),
            vmem(3, 5, 24, 40, 128),
            vmem(5, 16, 40, 128),
            *[vmem(count, tiles, 8, 128) for count in (6, 3, NY, NX) for tiles in (6, 5) for _ in range(2)],
            vmem(2, 3, 16, 8, 128),
            vmem(3, 2, 8, 128),
            vmem(3, 24, 128),
            vmem(3, 24, 128),
            vmem(5, 3, 16, 128),
            vmem(5, 2, 40, 128),
            vmem(3, 5, 2, 16, 128),
            vmem(5, 2, 16, 128),
            vmem(5, 2, 24, 128),
            vmem(5, 16, 128),
            vmem(5, 40, 128),
            vmem(5, 8, 16, 128),
            pltpu.SemaphoreType.DMA((2, 40)),
            pltpu.SemaphoreType.DMA((2, 40)),
            pltpu.SemaphoreType.DMA((3,)),
            pltpu.SemaphoreType.DMA((3,)),
            pltpu.SemaphoreType.DMA((6,)),
        ],
        compiler_params=pltpu.CompilerParams(collective_id=0, has_side_effects=True, vmem_limit_bytes=67043328),
        name="acoustic_steps",
    )(sector_offset, cell_shift, stencil_start, interface_fraction, mean_flow, acoustic_state)
    return without + ghosts


def solution(mesh):
    return jax.shard_map(
        shards,
        mesh=mesh,
        in_specs=(
            P(None, "azim", "rad", None),
            P(None, "rad", None),
            P(),
            P(None, "azim"),
            P(None, "azim"),
            P(None, "azim"),
        ),
        out_specs=P(None, "azim", "rad", None),
        check_vma=False,
    )
```

```python
import jax
import jax.numpy as jnp
from jax import lax
from jax.experimental import pallas as pl
from jax.experimental.pallas import tpu as pltpu
from jax.sharding import PartitionSpec as P

STENCIL = (0.841570125482, -0.244678631765, 0.059463584768, -0.007650904064)
STEP_SIZE = 0.2
MESH = pl.DeviceIdType.MESH
F32 = jnp.float32

NZ, NY, NX = 8, 4, 2
N = 128


def lanes(rows=8):
    return lax.broadcasted_iota(jnp.int32, (rows, 128), 1)


def moved(value, by):
    return value if by % 128 == 0 else pltpu.roll(value, (-by) % 128, value.ndim - 1)


def forcing(dx, dr, da):
    spread = dx[1] + dr[2] + da[3]
    return [spread, dx[4], dr[4], da[4], spread]


def kernel(offset_hbm, shift_hbm, start_hbm, fraction_hbm, flow_hbm, state_hbm, out_hbm, fix_hbm,
           offset_ref, shift_ref, start_ref, fraction_ref,
           E, mid, near_a0, near_a1, near_b0, near_b1, far_a0, far_a1, far_b0, far_b1, y_a0, y_a1, y_b0, y_b1, x_a0, x_a1, x_b0, x_b1, facing, own_coef, flow, flow_pack,
           own_pack, face_pad, slope, face_mid, own_fix, next_pack, fix_pad, wide_fix,
           send_sem, recv_sem, fixed_send, fixed_recv, local_sem):
    near_a, near_b, far_a, far_b = (near_a0, near_a1), (near_b0, near_b1), (far_a0, far_a1), (far_b0, far_b1)
    ys_a, ys_b, xs_a, xs_b = (y_a0, y_a1), (y_b0, y_b1), (x_a0, x_a1), (x_b0, x_b1)
    i = lax.axis_index("azim")
    r = lax.axis_index("rad")
    core, z, y, x = i % 2, (i // 2) % NZ, (i // 16) % NY, i // 64
    row0 = pl.multiple_of(8 + 8 * r, 8)
    far0 = pl.multiple_of(8 + 16 * r, 8)
    far0_here = pl.multiple_of(24 - 16 * r, 8)
    up, down = (i + 1) % N, (i + N - 1) % N

    def at(azim, rad=None):
        return {"azim": azim, "rad": r if rad is None else rad}

    def along_z(d):
        return i - 2 * z + 2 * ((z + d + NZ) % NZ)

    other = 1 - 2 * core
    near_to = [(i + other, 2 + core)]
    for d in (1, -1):
        near_to += [(along_z(d), 2 * (1 - d) + core), (along_z(d) + other, 2 * (1 - d) + core)]
    z_to = [(along_z(3), 0), (along_z(-3), 2)]
    y_to = [i - 16 * y + 16 * ((y + d) % NY) for d in (2, 1, 3)]
    x_to = (i + 64) % N

    loads = []

    def load(src, dst):
        copy = pltpu.make_async_copy(src, dst, local_sem.at[len(loads)])
        copy.start()
        loads.append(copy)

    load(state_hbm, E.at[0, :, pl.ds(8, 8), pl.ds(row0, 16), :])
    load(flow_hbm, flow.at[:, pl.ds(pl.multiple_of(8 * r, 8), 16), :])
    load(shift_hbm, shift_ref)
    load(start_hbm, start_ref)
    load(fraction_hbm, fraction_ref)
    load(offset_hbm, offset_ref)

    barrier = pltpu.get_barrier_semaphore()
    partners = [at(j) for j, _ in near_to] + [at(j) for j, _ in z_to] + [at(j) for j in y_to] + [at(x_to)]
    partners += [at(up), at(down), at(i, 1 - r), at(up, 1 - r), at(down, 1 - r)]
    for partner in partners:
        pl.semaphore_signal(barrier, inc=1, device_id=partner, device_id_type=MESH)

    edge = jnp.zeros((5, 16, 8, 128), F32)
    for n in range(2):
        E[n, :, 4:20, 0:8, :] = edge
        E[n, :, 4:20, 32:40, :] = edge
    for low in (0, 32):
        mid[:, :, low:low + 8, :] = edge
        face_pad[:, :, low:low + 8, :] = jnp.zeros((5, 2, 8, 128), F32)
        fix_pad[:, low:low + 8, :] = jnp.zeros((5, 8, 128), F32)

    lane = lanes()
    cell_of = (lane // 16 + 4) % 8
    upper = lane % 16 >= 8
    row = lax.broadcasted_iota(jnp.int32, (8, 128), 0)

    def spread_cells(get):
        value = jnp.full((8, 128), get(0))
        for a in range(1, 8):
            value = jnp.where(cell_of == a, get(a), value)
        return value

    def weights(t, m):
        up_one, down_one, down_two = t + 1.0, t - 1.0, t - 2.0
        w = (-t * down_one * down_two / 6.0, up_one * down_one * down_two / 2.0,
             -up_one * t * down_two / 2.0, up_one * t * down_one / 6.0)
        value = jnp.zeros((8, 128), F32)
        for p in range(4):
            value = jnp.where(m == p, w[p], value)
        return value

    def pack_rows(n, t, f):
        rows = pl.ds(pl.multiple_of(row0 + 8 * t, 8), 8)
        packed = None
        for a in range(8):
            turned = moved(E[n, f, 8 + a, rows, :], 56 - 16 * ((a + 4) % 8))
            packed = turned if packed is None else jnp.where(cell_of == a, turned, packed)
        return packed

    for copy in loads:
        copy.wait()
    for f in range(5):
        near_a[0][2 + core, f] = pack_rows(0, 0, f)
        ys_b[0][y, f] = pack_rows(0, 1, f)
    stator_t = spread_cells(lambda a: fraction_ref[0, a])
    rotor_t = spread_cells(lambda a: fraction_ref[1, a])
    for n in range(2):
        stator = weights(stator_t, row - spread_cells(lambda a: shift_ref[n, a] + start_ref[0, a] + 3))
        rotor = weights(rotor_t, row - spread_cells(lambda a: start_ref[1, a] - shift_ref[n, a]))
        own_coef[1, n] = jnp.where(upper, stator, rotor)
        near_a[n][2 + core, 5] = jnp.where(upper, rotor, stator)

    pl.semaphore_wait(barrier, len(partners))
    fixed = []

    def send_fixed(src, dst, to):
        no = len(fixed)
        copy = pltpu.make_async_remote_copy(src, dst, fixed_send.at[no], fixed_recv.at[no], device_id=to, device_id_type=MESH)
        copy.start()
        fixed.append(copy)

    half = lane % 64
    strip = lane % 16
    ahead = [jnp.where(half + j < 64, STENCIL[j - 1], 0.0) for j in range(1, 5)]
    behind = [jnp.where(half - j >= 0, STENCIL[j - 1], 0.0) for j in range(1, 5)]

    in_ahead = [jnp.where(strip % 8 + j < 8, STENCIL[j - 1], 0.0) for j in range(1, 5)]
    in_behind = [jnp.where(strip % 8 - j >= 0, STENCIL[j - 1], 0.0) for j in range(1, 5)]
    cross_ahead = [jnp.where((strip < 8) & (strip + j >= 8), STENCIL[j - 1], 0.0) for j in range(1, 5)]
    cross_behind = [jnp.where((strip >= 8) & (strip - j < 8), STENCIL[j - 1], 0.0) for j in range(1, 5)]

    def taps(value, fore, aft):
        total = None
        for j in range(1, 5):
            term = fore[j - 1][0:1] * moved(value, j) - aft[j - 1][0:1] * moved(value, -j)
            total = term if total is None else total + term
        return total

    def ring(sectors):
        low = lanes(sectors[0].shape[0]) < 64
        return [jnp.where(low, sectors[p], sectors[(p + 1) % 3]) for p in range(3)]

    def by_cells(packs, d):
        if d == 0:
            return packs[:2]
        at_lane = lanes(packs[0].shape[0])
        turned = [moved(v, 16 * d) for v in packs]
        if d > 0:
            return [jnp.where(at_lane < 128 - 16 * d, turned[p], turned[p + 1]) for p in range(2)]
        return [jnp.where(at_lane >= -16 * d, turned[p], turned[(p + 2) % 3]) for p in range(2)]

    def own_cells(packs, d):
        at_lane = lanes(packs[0].shape[0])
        first, last = (moved(v, 16 * d) for v in packs)
        if d >= 0:
            return jnp.where((at_lane >= 64) & (at_lane < 128 - 16 * d), first, last)
        return jnp.where((at_lane < 64) & (at_lane >= -16 * d), last, first)

    def evaluate_rows(ref, c, low):
        dx, dr, da, mine = [], [], [], []
        rows = pl.ds(low, 8)
        for f in range(5):
            here = ref[f, c, rows, :]
            mine.append(here)
            dx.append(taps(here, ahead, behind))
            radial = azimuthal = None
            for j in range(1, 5):
                step = STENCIL[j - 1] * (ref[f, c, pl.ds(low + j, 8), :] - ref[f, c, pl.ds(low - j, 8), :])
                radial = step if radial is None else radial + step
                step = STENCIL[j - 1] * (ref[f, c + j, rows, :] - ref[f, c - j, rows, :])
                azimuthal = step if azimuthal is None else azimuthal + step
            dr.append(radial)
            da.append(azimuthal)
        u = [flow[k, pl.ds(pl.multiple_of(low - 8, 8), 8), :] for k in range(3)]
        push = forcing(dx, dr, da)
        return mine, [-(u[0] * dx[f] + u[1] * dr[f] + u[2] * da[f]) - push[f] for f in range(5)]

    def radial_of(ref, *index):
        total = None
        for j in range(1, 5):
            part = STENCIL[j - 1] * (ref[(*index, slice(8 + j, 32 + j))] - ref[(*index, slice(8 - j, 32 - j))])
            total = part if total is None else total + part
        return total

    def own_rows_of(value):
        return jnp.where(r == 0, value[0:16], value[8:24])

    def widened(f, t, a):
        change = own_fix[f, 0, 8 * t:8 * t + 8, :]
        return jnp.where((lane >= 56) & (lane < 72), moved(change, 16 * ((a + 4) % 8) - 56), 0.0)

    def step(n):
        k = offset_ref[n]
        source_r = (i - k + N) % N
        source_s = (i + k) % N
        low_r = (core - k % 16 + 16) % 16
        low_s = (core + k % 16) % 16
        started = []

        def parts(low):
            far = ((low // 2 + 3) % 8 + 1) // 3 - 1
            near = (low // 2 + 3) % 8 - 3 - 3 * far
            return near, far

        def send(src, dst, to):
            no = len(started)
            copy = pltpu.make_async_remote_copy(src, dst, send_sem.at[n, no], recv_sem.at[n, no], device_id=to, device_id_type=MESH)
            copy.start()
            started.append(copy)
            return copy

        def chosen(slots, from_r, from_s):
            return jnp.where(upper[None], slots[from_r], slots[from_s])

        def along(slots, own, targets):
            mine = slots.at[own]
            return [send(mine, slots.at[place], at(j)) for j, place in targets]

        def arrived(copies):
            for copy in copies:
                copy.wait_recv()

        low = i % 16
        high = i // 16
        high_r = (high - k // 16 - (low + k % 16) // 16 + 16) % 8
        high_s = (high + k // 16 + (k % 16 + 15 - low) // 16) % 8
        (near_r, far_r), (near_s, far_s) = parts(low_r), parts(low_s)
        near_of = (2 * (near_r + 1) + low_r % 2, 2 * (near_s + 1) + low_s % 2)
        ys = [(j, y) for j in y_to]
        xs = [(x_to, x)]

        stage_a = along(near_a[n], 2 + core, near_to)
        stage_b = along(ys_b[n], y, ys)

        if n == 0:
            send_fixed(own_coef.at[1], own_coef.at[0], at(up))
            send_fixed(own_coef.at[1], own_coef.at[2], at(down))
            send_fixed(flow.at[:, pl.ds(8, 8), :], flow.at[:, pl.ds(pl.multiple_of(16 * r, 8), 8), :], at(i, 1 - r))
        else:
            def into_rows(f, carry):
                for t in range(2):
                    rows = pl.ds(pl.multiple_of(row0 + 8 * t, 8), 8)
                    for a in range(8):
                        E[1, f, 8 + a, rows, :] = E[1, f, 8 + a, rows, :] + widened(f, t, a)
                return carry

            lax.fori_loop(0, 5, into_rows, 0)

        own_rows, far_rows = pl.ds(row0, 16), pl.ds(far0, 8)
        halos = []

        def halo_cells(fields):
            part = E.at[n, fields, pl.ds(8, 8), own_rows, :]
            halos.append(send(part, E.at[n, fields, pl.ds(0, 8), own_rows, :], at(up)))
            halos.append(send(part, E.at[n, fields, pl.ds(16, 8), own_rows, :], at(down)))

        def halo_rows(fields):
            halos.append(send(E.at[n, fields, pl.ds(8, 8), pl.ds(16, 8), :], E.at[n, fields, pl.ds(8, 8), far_rows, :], at(i, 1 - r)))

        halo_rows(pl.ds(0, 3))
        halo_cells(pl.ds(0, 2))
        arrived(stage_a)
        far_a[n][1] = chosen(near_a[n], *near_of)
        stage_a = along(far_a[n], 1, z_to)
        arrived(stage_b)
        xs_b[n][x] = chosen(ys_b[n], high_r % NY, high_s % NY)
        stage_b = along(xs_b[n], x, xs)
        halo_cells(pl.ds(2, 2))

        arrived(stage_b)
        near_b[n][2 + core] = chosen(xs_b[n], high_r // NY, high_s // NY)
        stage_b = along(near_b[n], 2 + core, near_to)
        halo_rows(pl.ds(3, 2))
        halos.append(send(E.at[n, :, pl.ds(12, 4), pl.ds(16, 8), :], E.at[n, :, pl.ds(4, 4), far_rows, :], at(up, 1 - r)))
        halos.append(send(E.at[n, :, pl.ds(8, 4), pl.ds(16, 8), :], E.at[n, :, pl.ds(16, 4), far_rows, :], at(down, 1 - r)))
        arrived(stage_a)
        ys_a[n][y] = chosen(far_a[n], far_r + 1, far_s + 1)
        stage_a = along(ys_a[n], y, ys)
        halo_cells(pl.ds(4, 1))

        arrived(stage_b)
        far_b[n][1] = chosen(near_b[n], *near_of)
        stage_b = along(far_b[n], 1, z_to)
        arrived(stage_a)
        xs_a[n][x] = chosen(ys_a[n], (source_r // 16) % NY, (source_s // 16) % NY)
        stage_a = along(xs_a[n], x, xs)

        if n == 0:
            for copy in fixed:
                copy.wait()
            for m in range(3):
                packed = None
                for a in range(8):
                    turned = moved(flow[m], 56 - 16 * a)
                    packed = turned if packed is None else jnp.where(lanes(24) // 16 == a, turned, packed)
                flow_pack[m] = packed
        arrived(stage_a)
        got = chosen(xs_a[n], source_r // 64, source_s // 64)
        facing[n, 1, pl.ds(5 * r, 5)] = got[0:5]
        facing[n, 1, 15] = got[5]
        arrived(stage_b)
        facing[n, 1, pl.ds(5 * r + 5, 5)] = chosen(far_b[n], far_r + 1, far_s + 1)
        rows10, rows5 = pl.ds(5 * r, 10), pl.ds(10 * r, 5)
        stage = []
        for to, place in ((up, 0), (down, 2)):
            stage.append(send(facing.at[n, 1, rows10], facing.at[n, place, rows10], at(to)))
            stage.append(send(facing.at[n, 1, 15], facing.at[n, place, 15], at(to)))
            stage.append(send(facing.at[n, 1, pl.ds(5, 5)], facing.at[n, place, rows5], at(to, 1 - r)))
        stage.append(send(facing.at[n, 1, pl.ds(5, 5)], facing.at[n, 1, rows5], at(i, 1 - r)))

        for copy in halos:
            copy.wait_recv()

        def midpoint(c, low):
            here, slopes = evaluate_rows(E.at[n], c + 4, low)
            for f in range(5):
                mid[f, c, pl.ds(low, 8), :] = here[f] + (0.5 * STEP_SIZE) * slopes[f]

        def first(c, carry):
            midpoint(c, row0)
            midpoint(c, pl.multiple_of(row0 + 8, 8))
            return carry

        def first_far(c, carry):
            midpoint(c + 4, far0_here)
            return carry

        lax.fori_loop(0, 16, first, 0, unroll=2)
        lax.fori_loop(0, 8, first_far, 0, unroll=2)
        def second(c, carry):
            for t in range(2):
                low = pl.multiple_of(row0 + 8 * t, 8)
                _, slopes = evaluate_rows(mid, c + 4, low)
                for f in range(5):
                    E[n + 1, f, c + 8, pl.ds(low, 8), :] = E[n, f, c + 8, pl.ds(low, 8), :] + STEP_SIZE * slopes[f]
            return carry

        lax.fori_loop(0, 8, second, 0, unroll=2)
        if n == 1:
            pltpu.make_async_copy(*result, local_sem.at[0]).start()

        def strip_of(f, carry):
            for p in range(3):
                packed = None
                for a in range(8):
                    turned = moved(E[n, f, (4 + 8 * p + a) % 24, own_rows, :], 56 - 16 * a)
                    packed = turned if packed is None else jnp.where(lanes(16) // 16 == a, turned, packed)
                own_pack[f, p] = packed
            if n == 0:
                for t in range(2):
                    next_pack[f, 8 * t:8 * t + 8, :] = pack_rows(1, t, f)
            return carry

        lax.fori_loop(0, 5, strip_of, 0)
        coef_own = ring([own_coef[p, n] for p in range(3)])
        u24 = [flow_pack[m] for m in range(3)]
        u = [flow_pack[m, pl.ds(pl.multiple_of(8 * r, 8), 16), :] for m in range(3)]
        for copy in stage:
            copy.wait_recv()

        coef_face = ring([jnp.where(upper, moved(facing[n, p, 15], -8), moved(facing[n, p, 15], 8)) for p in range(3)])

        for f in range(5):
            F = ring([jnp.concatenate([facing[n, p, 5 * t + f] for t in range(3)], axis=0) for p in range(3)])
            M = [own_pack[f, p] for p in range(3)]
            F_own = [own_rows_of(v) for v in F]
            for p in range(2):
                face_pad[f, p, 8:32, :] = F[p]
            ghost_own = [jnp.zeros((24, 128), F32)] * 2
            ghost_face = [jnp.zeros((16, 128), F32)] * 2
            azimuthal = [jnp.zeros((16, 128), F32)] * 2
            for d in range(-4, 5):
                shifted = by_cells(F if d < 4 else F_own, d)
                if d < 4:
                    shifted_own = by_cells(M, d)
                for p in range(2):
                    if d != 0:
                        weight = STENCIL[d - 1] if d > 0 else -STENCIL[-d - 1]
                        azimuthal[p] = azimuthal[p] + weight * (own_rows_of(shifted[p]) if d < 4 else shifted[p])
                    if d < 4:
                        ghost_own[p] = ghost_own[p] + coef_own[p][d + 4:d + 5, :] * shifted[p]
                        ghost_face[p] = ghost_face[p] + coef_face[p][d + 4:d + 5, :] * shifted_own[p]
            for p in range(2):
                slope[0, f, p] = taps(F_own[p], in_ahead, in_behind) + taps(ghost_face[p], cross_ahead, cross_behind)
                slope[1, f, p] = own_rows_of(radial_of(face_pad, f, p))
                slope[2, f, p] = azimuthal[p]
                own_fix[f, p] = taps(ghost_own[p], cross_ahead, cross_behind)

        for p in range(2):
            dx, dr, da = ([slope[m, f, p] for f in range(5)] for m in range(3))
            push = forcing(dx, dr, da)
            for f in range(5):
                change = -(u[0] * dx[f] + u[1] * dr[f] + u[2] * da[f]) - push[f]
                face_mid[f, p] = face_pad[f, p, own_rows, :] + (0.5 * STEP_SIZE) * change
            cut = [own_fix[f, p] for f in range(5)]
            push = [cut[1], cut[4], 0.0, 0.0, cut[1]]
            for f in range(5):
                own_fix[f, p] = (-0.5 * STEP_SIZE) * (u24[0] * cut[f] + push[f])

        for f in range(5):
            face = [face_mid[f, p] for p in range(2)]
            fix = [own_rows_of(own_fix[f, p]) for p in range(2)]
            fix_pad[f, 8:32, :] = own_cells([own_fix[f, p] for p in range(2)], 0)
            ghosts = jnp.zeros((16, 128), F32)
            azimuthal = jnp.zeros((16, 128), F32)
            for d in range(-4, 5):
                if d < 4:
                    ghosts = ghosts + own_coef[1, n, d + 4:d + 5, :] * own_cells(face, d)
                if d != 0:
                    weight = STENCIL[d - 1] if d > 0 else -STENCIL[-d - 1]
                    azimuthal = azimuthal + weight * own_cells(fix, d)
            slope[0, f, 0] = taps(own_cells(fix, 0), in_ahead, in_behind) + taps(ghosts, cross_ahead, cross_behind)
            slope[1, f, 0] = own_rows_of(radial_of(fix_pad, f))
            slope[2, f, 0] = azimuthal
        dx, dr, da = ([slope[m, f, 0] for f in range(5)] for m in range(3))
        push = forcing(dx, dr, da)
        for f in range(5):
            change = -STEP_SIZE * (u[0] * dx[f] + u[1] * dr[f] + u[2] * da[f] + push[f])
            own_fix[f, 0, 0:16, :] = change
            if n == 0:
                after = next_pack[f] + change
                near_a[1][2 + core, f] = after[0:8]
                ys_b[1][y, f] = after[8:16]
        return started

    result = (E.at[2, :, pl.ds(8, 8), pl.ds(row0, 16), :], out_hbm)
    started = step(0)
    started += step(1)

    def into_fix(f, carry):
        for t in range(2):
            for a in range(8):
                wide_fix[f, a, 8 * t:8 * t + 8, :] = widened(f, t, a)
        return carry

    lax.fori_loop(0, 5, into_fix, 0)
    store_fix = pltpu.make_async_copy(wide_fix, fix_hbm, local_sem.at[1])
    store_fix.start()
    for copy in started:
        copy.wait_send()
    pltpu.make_async_copy(*result, local_sem.at[0]).wait()
    store_fix.wait()


def shards(acoustic_state, mean_flow, sector_offset, cell_shift, stencil_start, interface_fraction):
    anywhere = pl.BlockSpec(memory_space=pl.ANY)
    vmem = lambda *shape: pltpu.VMEM(shape, F32)
    smem = lambda value: pltpu.SMEM(value.shape, value.dtype)
    without, ghosts = pl.pallas_call(
        kernel,
        out_shape=[jax.ShapeDtypeStruct(acoustic_state.shape, F32)] * 2,
        in_specs=[anywhere] * 6,
        out_specs=[anywhere] * 2,
        scratch_shapes=[
            smem(sector_offset),
            smem(cell_shift),
            smem(stencil_start),
            smem(interface_fraction),
            vmem(3, 5, 24, 40, 128),
            vmem(5, 16, 40, 128),
            *[vmem(count, tiles, 8, 128) for count in (6, 3, NY, NX) for tiles in (6, 5) for _ in range(2)],
            vmem(2, 3, 16, 8, 128),
            vmem(3, 2, 8, 128),
            vmem(3, 24, 128),
            vmem(3, 24, 128),
            vmem(5, 3, 16, 128),
            vmem(5, 2, 40, 128),
            vmem(3, 5, 2, 16, 128),
            vmem(5, 2, 16, 128),
            vmem(5, 2, 24, 128),
            vmem(5, 16, 128),
            vmem(5, 40, 128),
            vmem(5, 8, 16, 128),
            pltpu.SemaphoreType.DMA((2, 40)),
            pltpu.SemaphoreType.DMA((2, 40)),
            pltpu.SemaphoreType.DMA((3,)),
            pltpu.SemaphoreType.DMA((3,)),
            pltpu.SemaphoreType.DMA((6,)),
        ],
        compiler_params=pltpu.CompilerParams(collective_id=0, has_side_effects=True, vmem_limit_bytes=67043328),
        name="acoustic_steps",
    )(sector_offset, cell_shift, stencil_start, interface_fraction, mean_flow, acoustic_state)
    return without + ghosts


def solution(mesh):
    return jax.shard_map(
        shards,
        mesh=mesh,
        in_specs=(
            P(None, "azim", "rad", None),
            P(None, "rad", None),
            P(),
            P(None, "azim"),
            P(None, "azim"),
            P(None, "azim"),
        ),
        out_specs=P(None, "azim", "rad", None),
        check_vma=False,
    )
```

```python
import jax
import jax.numpy as jnp
from jax import lax
from jax.experimental import pallas as pl
from jax.experimental.pallas import tpu as pltpu
from jax.sharding import PartitionSpec as P

STENCIL = (0.841570125482, -0.244678631765, 0.059463584768, -0.007650904064)
STEP_SIZE = 0.2
MESH = pl.DeviceIdType.MESH
F32 = jnp.float32

NZ, NY, NX = 8, 4, 2
N = 128


def lanes(rows=8):
    return lax.broadcasted_iota(jnp.int32, (rows, 128), 1)


def moved(value, by):
    return value if by % 128 == 0 else pltpu.roll(value, (-by) % 128, value.ndim - 1)


def forcing(dx, dr, da):
    spread = dx[1] + dr[2] + da[3]
    return [spread, dx[4], dr[4], da[4], spread]


def kernel(offset_hbm, shift_hbm, start_hbm, fraction_hbm, flow_hbm, state_hbm, out_hbm, fix_hbm,
           offset_ref, shift_ref, start_ref, fraction_ref,
           E, mid, near_a0, near_a1, near_b0, near_b1, far_a0, far_a1, far_b0, far_b1, y_a0, y_a1, y_b0, y_b1, x_a0, x_a1, x_b0, x_b1, facing, own_coef, flow, flow_pack,
           own_pack, face_pad, slope, face_mid, own_fix, next_pack, fix_pad, wide_fix, inside, across,
           send_sem, recv_sem, fixed_send, fixed_recv, local_sem):
    near_a, near_b, far_a, far_b = (near_a0, near_a1), (near_b0, near_b1), (far_a0, far_a1), (far_b0, far_b1)
    ys_a, ys_b, xs_a, xs_b = (y_a0, y_a1), (y_b0, y_b1), (x_a0, x_a1), (x_b0, x_b1)
    i = lax.axis_index("azim")
    r = lax.axis_index("rad")
    core, z, y, x = i % 2, (i // 2) % NZ, (i // 16) % NY, i // 64
    row0 = pl.multiple_of(8 + 8 * r, 8)
    far0 = pl.multiple_of(8 + 16 * r, 8)
    far0_here = pl.multiple_of(24 - 16 * r, 8)
    up, down = (i + 1) % N, (i + N - 1) % N

    def at(azim, rad=None):
        return {"azim": azim, "rad": r if rad is None else rad}

    def along_z(d):
        return i - 2 * z + 2 * ((z + d + NZ) % NZ)

    other = 1 - 2 * core
    near_to = [(i + other, 2 + core)]
    for d in (1, -1):
        near_to += [(along_z(d), 2 * (1 - d) + core), (along_z(d) + other, 2 * (1 - d) + core)]
    z_to = [(along_z(3), 0), (along_z(-3), 2)]
    y_to = [i - 16 * y + 16 * ((y + d) % NY) for d in (2, 1, 3)]
    x_to = (i + 64) % N

    loads = []

    def load(src, dst):
        copy = pltpu.make_async_copy(src, dst, local_sem.at[len(loads)])
        copy.start()
        loads.append(copy)

    load(state_hbm, E.at[0, :, pl.ds(8, 8), pl.ds(row0, 16), :])
    load(flow_hbm, flow.at[:, pl.ds(pl.multiple_of(8 * r, 8), 16), :])
    load(shift_hbm, shift_ref)
    load(start_hbm, start_ref)
    load(fraction_hbm, fraction_ref)
    load(offset_hbm, offset_ref)

    barrier = pltpu.get_barrier_semaphore()
    partners = [at(j) for j, _ in near_to] + [at(j) for j, _ in z_to] + [at(j) for j in y_to] + [at(x_to)]
    partners += [at(up), at(down), at(i, 1 - r), at(up, 1 - r), at(down, 1 - r)]
    for partner in partners:
        pl.semaphore_signal(barrier, inc=1, device_id=partner, device_id_type=MESH)

    edge = jnp.zeros((5, 16, 8, 128), F32)
    for n in range(2):
        E[n, :, 4:20, 0:8, :] = edge
        E[n, :, 4:20, 32:40, :] = edge
    for low in (0, 32):
        mid[:, :, low:low + 8, :] = edge
        face_pad[:, :, low:low + 8, :] = jnp.zeros((5, 2, 8, 128), F32)
        fix_pad[:, low:low + 8, :] = jnp.zeros((5, 8, 128), F32)

    source = lax.broadcasted_iota(jnp.int32, (128, 128), 0)
    target = lax.broadcasted_iota(jnp.int32, (128, 128), 1)
    weight = jnp.zeros((128, 128), F32)
    for j in range(1, 5):
        weight = jnp.where(source - target == j, STENCIL[j - 1], jnp.where(target - source == j, -STENCIL[j - 1], weight))
    same_cell = source // 16 == target // 16
    same_frame = source // 8 == target // 8
    inside[...] = jnp.where(same_frame, weight, 0.0)
    across[...] = jnp.where(same_cell & ~same_frame, weight, 0.0)

    lane = lanes()
    cell_of = (lane // 16 + 4) % 8
    upper = lane % 16 >= 8
    row = lax.broadcasted_iota(jnp.int32, (8, 128), 0)

    def spread_cells(get):
        value = jnp.full((8, 128), get(0))
        for a in range(1, 8):
            value = jnp.where(cell_of == a, get(a), value)
        return value

    def weights(t, m):
        up_one, down_one, down_two = t + 1.0, t - 1.0, t - 2.0
        w = (-t * down_one * down_two / 6.0, up_one * down_one * down_two / 2.0,
             -up_one * t * down_two / 2.0, up_one * t * down_one / 6.0)
        value = jnp.zeros((8, 128), F32)
        for p in range(4):
            value = jnp.where(m == p, w[p], value)
        return value

    def pack_rows(n, t, f):
        rows = pl.ds(pl.multiple_of(row0 + 8 * t, 8), 8)
        packed = None
        for a in range(8):
            turned = moved(E[n, f, 8 + a, rows, :], 56 - 16 * ((a + 4) % 8))
            packed = turned if packed is None else jnp.where(cell_of == a, turned, packed)
        return packed

    for copy in loads:
        copy.wait()
    for f in range(5):
        near_a[0][2 + core, f] = pack_rows(0, 0, f)
        ys_b[0][y, f] = pack_rows(0, 1, f)
    stator_t = spread_cells(lambda a: fraction_ref[0, a])
    rotor_t = spread_cells(lambda a: fraction_ref[1, a])
    for n in range(2):
        stator = weights(stator_t, row - spread_cells(lambda a: shift_ref[n, a] + start_ref[0, a] + 3))
        rotor = weights(rotor_t, row - spread_cells(lambda a: start_ref[1, a] - shift_ref[n, a]))
        own_coef[1, n] = jnp.where(upper, stator, rotor)
        near_a[n][2 + core, 5] = jnp.where(upper, rotor, stator)

    pl.semaphore_wait(barrier, len(partners))
    fixed = []

    def send_fixed(src, dst, to):
        no = len(fixed)
        copy = pltpu.make_async_remote_copy(src, dst, fixed_send.at[no], fixed_recv.at[no], device_id=to, device_id_type=MESH)
        copy.start()
        fixed.append(copy)

    half = lane % 64
    ahead = [jnp.where(half + j < 64, STENCIL[j - 1], 0.0) for j in range(1, 5)]
    behind = [jnp.where(half - j >= 0, STENCIL[j - 1], 0.0) for j in range(1, 5)]

    def taps(value, fore, aft):
        total = None
        for j in range(1, 5):
            term = fore[j - 1][0:1] * moved(value, j) - aft[j - 1][0:1] * moved(value, -j)
            total = term if total is None else total + term
        return total

    def product(parts, matrix):
        rows = parts[0].shape[0]
        whole = jnp.dot(jnp.concatenate(parts, axis=0), matrix[...], precision=lax.Precision.HIGHEST, preferred_element_type=F32)
        return [whole[rows * m:rows * m + rows] for m in range(len(parts))]

    def ring(sectors):
        low = lanes(sectors[0].shape[0]) < 64
        return [jnp.where(low, sectors[p], sectors[(p + 1) % 3]) for p in range(3)]

    def by_cells(packs, d):
        if d == 0:
            return packs[:2]
        at_lane = lanes(packs[0].shape[0])
        turned = [moved(v, 16 * d) for v in packs]
        if d > 0:
            return [jnp.where(at_lane < 128 - 16 * d, turned[p], turned[p + 1]) for p in range(2)]
        return [jnp.where(at_lane >= -16 * d, turned[p], turned[(p + 2) % 3]) for p in range(2)]

    def own_cells(packs, d):
        at_lane = lanes(packs[0].shape[0])
        first, last = (moved(v, 16 * d) for v in packs)
        if d >= 0:
            return jnp.where((at_lane >= 64) & (at_lane < 128 - 16 * d), first, last)
        return jnp.where((at_lane < 64) & (at_lane >= -16 * d), last, first)

    def evaluate_rows(ref, c, low):
        dx, dr, da, mine = [], [], [], []
        rows = pl.ds(low, 8)
        for f in range(5):
            here = ref[f, c, rows, :]
            mine.append(here)
            dx.append(taps(here, ahead, behind))
            radial = azimuthal = None
            for j in range(1, 5):
                step = STENCIL[j - 1] * (ref[f, c, pl.ds(low + j, 8), :] - ref[f, c, pl.ds(low - j, 8), :])
                radial = step if radial is None else radial + step
                step = STENCIL[j - 1] * (ref[f, c + j, rows, :] - ref[f, c - j, rows, :])
                azimuthal = step if azimuthal is None else azimuthal + step
            dr.append(radial)
            da.append(azimuthal)
        u = [flow[k, pl.ds(pl.multiple_of(low - 8, 8), 8), :] for k in range(3)]
        push = forcing(dx, dr, da)
        return mine, [-(u[0] * dx[f] + u[1] * dr[f] + u[2] * da[f]) - push[f] for f in range(5)]

    def radial_of(ref, *index):
        total = None
        for j in range(1, 5):
            part = STENCIL[j - 1] * (ref[(*index, slice(8 + j, 32 + j))] - ref[(*index, slice(8 - j, 32 - j))])
            total = part if total is None else total + part
        return total

    def own_rows_of(value):
        return jnp.where(r == 0, value[0:16], value[8:24])

    def widened(f, t, a):
        change = own_fix[f, 0, 8 * t:8 * t + 8, :]
        return jnp.where((lane >= 56) & (lane < 72), moved(change, 16 * ((a + 4) % 8) - 56), 0.0)

    def step(n):
        k = offset_ref[n]
        source_r = (i - k + N) % N
        source_s = (i + k) % N
        low_r = (core - k % 16 + 16) % 16
        low_s = (core + k % 16) % 16
        started = []

        def parts(low):
            far = ((low // 2 + 3) % 8 + 1) // 3 - 1
            near = (low // 2 + 3) % 8 - 3 - 3 * far
            return near, far

        def send(src, dst, to):
            no = len(started)
            copy = pltpu.make_async_remote_copy(src, dst, send_sem.at[n, no], recv_sem.at[n, no], device_id=to, device_id_type=MESH)
            copy.start()
            started.append(copy)
            return copy

        def chosen(slots, from_r, from_s):
            return jnp.where(upper[None], slots[from_r], slots[from_s])

        def along(slots, own, targets):
            mine = slots.at[own]
            return [send(mine, slots.at[place], at(j)) for j, place in targets]

        def arrived(copies):
            for copy in copies:
                copy.wait_recv()

        low = i % 16
        high = i // 16
        high_r = (high - k // 16 - (low + k % 16) // 16 + 16) % 8
        high_s = (high + k // 16 + (k % 16 + 15 - low) // 16) % 8
        (near_r, far_r), (near_s, far_s) = parts(low_r), parts(low_s)
        near_of = (2 * (near_r + 1) + low_r % 2, 2 * (near_s + 1) + low_s % 2)
        ys = [(j, y) for j in y_to]
        xs = [(x_to, x)]

        stage_a = along(near_a[n], 2 + core, near_to)
        stage_b = along(ys_b[n], y, ys)

        if n == 0:
            send_fixed(own_coef.at[1], own_coef.at[0], at(up))
            send_fixed(own_coef.at[1], own_coef.at[2], at(down))
            send_fixed(flow.at[:, pl.ds(8, 8), :], flow.at[:, pl.ds(pl.multiple_of(16 * r, 8), 8), :], at(i, 1 - r))
        else:
            def into_rows(f, carry):
                for t in range(2):
                    rows = pl.ds(pl.multiple_of(row0 + 8 * t, 8), 8)
                    for a in range(8):
                        E[1, f, 8 + a, rows, :] = E[1, f, 8 + a, rows, :] + widened(f, t, a)
                return carry

            lax.fori_loop(0, 5, into_rows, 0)

        own_rows, far_rows = pl.ds(row0, 16), pl.ds(far0, 8)
        halos = []

        def halo_cells(fields):
            part = E.at[n, fields, pl.ds(8, 8), own_rows, :]
            halos.append(send(part, E.at[n, fields, pl.ds(0, 8), own_rows, :], at(up)))
            halos.append(send(part, E.at[n, fields, pl.ds(16, 8), own_rows, :], at(down)))

        def halo_rows(fields):
            halos.append(send(E.at[n, fields, pl.ds(8, 8), pl.ds(16, 8), :], E.at[n, fields, pl.ds(8, 8), far_rows, :], at(i, 1 - r)))

        halo_rows(pl.ds(0, 3))
        halo_cells(pl.ds(0, 2))
        arrived(stage_a)
        far_a[n][1] = chosen(near_a[n], *near_of)
        stage_a = along(far_a[n], 1, z_to)
        arrived(stage_b)
        xs_b[n][x] = chosen(ys_b[n], high_r % NY, high_s % NY)
        stage_b = along(xs_b[n], x, xs)
        halo_cells(pl.ds(2, 2))

        arrived(stage_b)
        near_b[n][2 + core] = chosen(xs_b[n], high_r // NY, high_s // NY)
        stage_b = along(near_b[n], 2 + core, near_to)
        halo_rows(pl.ds(3, 2))
        halos.append(send(E.at[n, :, pl.ds(12, 4), pl.ds(16, 8), :], E.at[n, :, pl.ds(4, 4), far_rows, :], at(up, 1 - r)))
        halos.append(send(E.at[n, :, pl.ds(8, 4), pl.ds(16, 8), :], E.at[n, :, pl.ds(16, 4), far_rows, :], at(down, 1 - r)))
        arrived(stage_a)
        ys_a[n][y] = chosen(far_a[n], far_r + 1, far_s + 1)
        stage_a = along(ys_a[n], y, ys)
        halo_cells(pl.ds(4, 1))

        arrived(stage_b)
        far_b[n][1] = chosen(near_b[n], *near_of)
        stage_b = along(far_b[n], 1, z_to)
        arrived(stage_a)
        xs_a[n][x] = chosen(ys_a[n], (source_r // 16) % NY, (source_s // 16) % NY)
        stage_a = along(xs_a[n], x, xs)

        if n == 0:
            for copy in fixed:
                copy.wait()
            for m in range(3):
                packed = None
                for a in range(8):
                    turned = moved(flow[m], 56 - 16 * a)
                    packed = turned if packed is None else jnp.where(lanes(24) // 16 == a, turned, packed)
                flow_pack[m] = packed
        arrived(stage_a)
        got = chosen(xs_a[n], source_r // 64, source_s // 64)
        facing[n, 1, pl.ds(5 * r, 5)] = got[0:5]
        facing[n, 1, 15] = got[5]
        arrived(stage_b)
        facing[n, 1, pl.ds(5 * r + 5, 5)] = chosen(far_b[n], far_r + 1, far_s + 1)
        rows10, rows5 = pl.ds(5 * r, 10), pl.ds(10 * r, 5)
        stage = []
        for to, place in ((up, 0), (down, 2)):
            stage.append(send(facing.at[n, 1, rows10], facing.at[n, place, rows10], at(to)))
            stage.append(send(facing.at[n, 1, 15], facing.at[n, place, 15], at(to)))
            stage.append(send(facing.at[n, 1, pl.ds(5, 5)], facing.at[n, place, rows5], at(to, 1 - r)))
        stage.append(send(facing.at[n, 1, pl.ds(5, 5)], facing.at[n, 1, rows5], at(i, 1 - r)))

        for copy in halos:
            copy.wait_recv()

        def midpoint(c, low):
            here, slopes = evaluate_rows(E.at[n], c + 4, low)
            for f in range(5):
                mid[f, c, pl.ds(low, 8), :] = here[f] + (0.5 * STEP_SIZE) * slopes[f]

        def first(c, carry):
            midpoint(c, row0)
            midpoint(c, pl.multiple_of(row0 + 8, 8))
            return carry

        def first_far(c, carry):
            midpoint(c + 4, far0_here)
            return carry

        lax.fori_loop(0, 16, first, 0, unroll=2)
        lax.fori_loop(0, 8, first_far, 0, unroll=2)
        def second(c, carry):
            for t in range(2):
                low = pl.multiple_of(row0 + 8 * t, 8)
                _, slopes = evaluate_rows(mid, c + 4, low)
                for f in range(5):
                    E[n + 1, f, c + 8, pl.ds(low, 8), :] = E[n, f, c + 8, pl.ds(low, 8), :] + STEP_SIZE * slopes[f]
            return carry

        lax.fori_loop(0, 8, second, 0, unroll=2)
        if n == 1:
            pltpu.make_async_copy(*result, local_sem.at[0]).start()

        def strip_of(f, carry):
            for p in range(3):
                packed = None
                for a in range(8):
                    turned = moved(E[n, f, (4 + 8 * p + a) % 24, own_rows, :], 56 - 16 * a)
                    packed = turned if packed is None else jnp.where(lanes(16) // 16 == a, turned, packed)
                own_pack[f, p] = packed
            if n == 0:
                for t in range(2):
                    next_pack[f, 8 * t:8 * t + 8, :] = pack_rows(1, t, f)
            return carry

        lax.fori_loop(0, 5, strip_of, 0)
        coef_own = ring([own_coef[p, n] for p in range(3)])
        u24 = [flow_pack[m] for m in range(3)]
        u = [flow_pack[m, pl.ds(pl.multiple_of(8 * r, 8), 16), :] for m in range(3)]
        for copy in stage:
            copy.wait_recv()

        coef_face = ring([jnp.where(upper, moved(facing[n, p, 15], -8), moved(facing[n, p, 15], 8)) for p in range(3)])

        all_face, all_ghost_own, all_ghost_face = [], [], []
        for f in range(5):
            F = ring([jnp.concatenate([facing[n, p, 5 * t + f] for t in range(3)], axis=0) for p in range(3)])
            M = [own_pack[f, p] for p in range(3)]
            F_own = [own_rows_of(v) for v in F]
            for p in range(2):
                face_pad[f, p, 8:32, :] = F[p]
            ghost_own = [jnp.zeros((24, 128), F32)] * 2
            ghost_face = [jnp.zeros((16, 128), F32)] * 2
            azimuthal = [jnp.zeros((16, 128), F32)] * 2
            for d in range(-4, 5):
                shifted = by_cells(F if d < 4 else F_own, d)
                if d < 4:
                    shifted_own = by_cells(M, d)
                for p in range(2):
                    if d != 0:
                        weight = STENCIL[d - 1] if d > 0 else -STENCIL[-d - 1]
                        azimuthal[p] = azimuthal[p] + weight * (own_rows_of(shifted[p]) if d < 4 else shifted[p])
                    if d < 4:
                        ghost_own[p] = ghost_own[p] + coef_own[p][d + 4:d + 5, :] * shifted[p]
                        ghost_face[p] = ghost_face[p] + coef_face[p][d + 4:d + 5, :] * shifted_own[p]
            for p in range(2):
                slope[1, f, p] = own_rows_of(radial_of(face_pad, f, p))
                slope[2, f, p] = azimuthal[p]
            all_face += F_own[:2]
            all_ghost_own += ghost_own
            all_ghost_face += ghost_face
        for m, (a, b) in enumerate(zip(product(all_face, inside), product(all_ghost_face, across))):
            slope[0, m // 2, m % 2] = a + b
        for m, a in enumerate(product(all_ghost_own, across)):
            own_fix[m // 2, m % 2] = a

        for p in range(2):
            dx, dr, da = ([slope[m, f, p] for f in range(5)] for m in range(3))
            push = forcing(dx, dr, da)
            for f in range(5):
                change = -(u[0] * dx[f] + u[1] * dr[f] + u[2] * da[f]) - push[f]
                face_mid[f, p] = face_pad[f, p, own_rows, :] + (0.5 * STEP_SIZE) * change
            cut = [own_fix[f, p] for f in range(5)]
            push = [cut[1], cut[4], 0.0, 0.0, cut[1]]
            for f in range(5):
                own_fix[f, p] = (-0.5 * STEP_SIZE) * (u24[0] * cut[f] + push[f])

        all_fix, all_ghost = [], []
        for f in range(5):
            face = [face_mid[f, p] for p in range(2)]
            fix = [own_rows_of(own_fix[f, p]) for p in range(2)]
            fix_pad[f, 8:32, :] = own_cells([own_fix[f, p] for p in range(2)], 0)
            ghosts = jnp.zeros((16, 128), F32)
            azimuthal = jnp.zeros((16, 128), F32)
            for d in range(-4, 5):
                if d < 4:
                    ghosts = ghosts + own_coef[1, n, d + 4:d + 5, :] * own_cells(face, d)
                if d != 0:
                    weight = STENCIL[d - 1] if d > 0 else -STENCIL[-d - 1]
                    azimuthal = azimuthal + weight * own_cells(fix, d)
            all_fix.append(own_cells(fix, 0))
            all_ghost.append(ghosts)
            slope[1, f, 0] = own_rows_of(radial_of(fix_pad, f))
            slope[2, f, 0] = azimuthal
        dx = [a + b for a, b in zip(product(all_fix, inside), product(all_ghost, across))]
        dr, da = ([slope[m, f, 0] for f in range(5)] for m in range(1, 3))
        push = forcing(dx, dr, da)
        for f in range(5):
            change = -STEP_SIZE * (u[0] * dx[f] + u[1] * dr[f] + u[2] * da[f] + push[f])
            own_fix[f, 0, 0:16, :] = change
            if n == 0:
                after = next_pack[f] + change
                near_a[1][2 + core, f] = after[0:8]
                ys_b[1][y, f] = after[8:16]
        return started

    result = (E.at[2, :, pl.ds(8, 8), pl.ds(row0, 16), :], out_hbm)
    started = step(0)
    started += step(1)

    def into_fix(f, carry):
        for t in range(2):
            for a in range(8):
                wide_fix[f, a, 8 * t:8 * t + 8, :] = widened(f, t, a)
        return carry

    lax.fori_loop(0, 5, into_fix, 0)
    store_fix = pltpu.make_async_copy(wide_fix, fix_hbm, local_sem.at[1])
    store_fix.start()
    for copy in started:
        copy.wait_send()
    pltpu.make_async_copy(*result, local_sem.at[0]).wait()
    store_fix.wait()


def shards(acoustic_state, mean_flow, sector_offset, cell_shift, stencil_start, interface_fraction):
    anywhere = pl.BlockSpec(memory_space=pl.ANY)
    vmem = lambda *shape: pltpu.VMEM(shape, F32)
    smem = lambda value: pltpu.SMEM(value.shape, value.dtype)
    without, ghosts = pl.pallas_call(
        kernel,
        out_shape=[jax.ShapeDtypeStruct(acoustic_state.shape, F32)] * 2,
        in_specs=[anywhere] * 6,
        out_specs=[anywhere] * 2,
        scratch_shapes=[
            smem(sector_offset),
            smem(cell_shift),
            smem(stencil_start),
            smem(interface_fraction),
            vmem(3, 5, 24, 40, 128),
            vmem(5, 16, 40, 128),
            *[vmem(count, tiles, 8, 128) for count in (6, 3, NY, NX) for tiles in (6, 5) for _ in range(2)],
            vmem(2, 3, 16, 8, 128),
            vmem(3, 2, 8, 128),
            vmem(3, 24, 128),
            vmem(3, 24, 128),
            vmem(5, 3, 16, 128),
            vmem(5, 2, 40, 128),
            vmem(3, 5, 2, 16, 128),
            vmem(5, 2, 16, 128),
            vmem(5, 2, 24, 128),
            vmem(5, 16, 128),
            vmem(5, 40, 128),
            vmem(5, 8, 16, 128),
            vmem(128, 128),
            vmem(128, 128),
            pltpu.SemaphoreType.DMA((2, 40)),
            pltpu.SemaphoreType.DMA((2, 40)),
            pltpu.SemaphoreType.DMA((3,)),
            pltpu.SemaphoreType.DMA((3,)),
            pltpu.SemaphoreType.DMA((6,)),
        ],
        compiler_params=pltpu.CompilerParams(collective_id=0, has_side_effects=True, vmem_limit_bytes=67043328),
        name="acoustic_steps",
    )(sector_offset, cell_shift, stencil_start, interface_fraction, mean_flow, acoustic_state)
    return without + ghosts


def solution(mesh):
    return jax.shard_map(
        shards,
        mesh=mesh,
        in_specs=(
            P(None, "azim", "rad", None),
            P(None, "rad", None),
            P(),
            P(None, "azim"),
            P(None, "azim"),
            P(None, "azim"),
        ),
        out_specs=P(None, "azim", "rad", None),
        check_vma=False,
    )
```

```python
import jax
import jax.numpy as jnp
from jax import lax
from jax.experimental import pallas as pl
from jax.experimental.pallas import tpu as pltpu
from jax.sharding import PartitionSpec as P

STENCIL = (0.841570125482, -0.244678631765, 0.059463584768, -0.007650904064)
STEP_SIZE = 0.2
MESH = pl.DeviceIdType.MESH
F32 = jnp.float32

NZ, NY, NX = 8, 4, 2
N = 128


def lanes(rows=8):
    return lax.broadcasted_iota(jnp.int32, (rows, 128), 1)


def moved(value, by):
    return value if by % 128 == 0 else pltpu.roll(value, (-by) % 128, value.ndim - 1)


def forcing(dx, dr, da):
    spread = dx[1] + dr[2] + da[3]
    return [spread, dx[4], dr[4], da[4], spread]


def kernel(offset_hbm, shift_hbm, start_hbm, fraction_hbm, flow_hbm, state_hbm, out_hbm, fix_hbm,
           offset_ref, shift_ref, start_ref, fraction_ref,
           E, mid, near_a0, near_a1, near_b0, near_b1, far_a0, far_a1, far_b0, far_b1, y_a0, y_a1, y_b0, y_b1, x_a0, x_a1, x_b0, x_b1, facing, own_coef, flow, flow_pack,
           face_pad, slope, face_mid, own_fix, next_pack, fix_pad, wide_fix, inside, across, own_shifted,
           send_sem, recv_sem, fixed_send, fixed_recv, local_sem):
    near_a, near_b, far_a, far_b = (near_a0, near_a1), (near_b0, near_b1), (far_a0, far_a1), (far_b0, far_b1)
    ys_a, ys_b, xs_a, xs_b = (y_a0, y_a1), (y_b0, y_b1), (x_a0, x_a1), (x_b0, x_b1)
    i = lax.axis_index("azim")
    r = lax.axis_index("rad")
    core, z, y, x = i % 2, (i // 2) % NZ, (i // 16) % NY, i // 64
    row0 = pl.multiple_of(8 + 8 * r, 8)
    far0 = pl.multiple_of(8 + 16 * r, 8)
    far0_here = pl.multiple_of(24 - 16 * r, 8)
    up, down = (i + 1) % N, (i + N - 1) % N

    def at(azim, rad=None):
        return {"azim": azim, "rad": r if rad is None else rad}

    def along_z(d):
        return i - 2 * z + 2 * ((z + d + NZ) % NZ)

    other = 1 - 2 * core
    near_to = [(i + other, 2 + core)]
    for d in (1, -1):
        near_to += [(along_z(d), 2 * (1 - d) + core), (along_z(d) + other, 2 * (1 - d) + core)]
    z_to = [(along_z(3), 0), (along_z(-3), 2)]
    y_to = [i - 16 * y + 16 * ((y + d) % NY) for d in (2, 1, 3)]
    x_to = (i + 64) % N

    loads = []

    def load(src, dst):
        copy = pltpu.make_async_copy(src, dst, local_sem.at[len(loads)])
        copy.start()
        loads.append(copy)

    load(state_hbm, E.at[0, :, pl.ds(8, 8), pl.ds(row0, 16), :])
    load(flow_hbm, flow.at[:, pl.ds(pl.multiple_of(8 * r, 8), 16), :])
    load(shift_hbm, shift_ref)
    load(start_hbm, start_ref)
    load(fraction_hbm, fraction_ref)
    load(offset_hbm, offset_ref)

    barrier = pltpu.get_barrier_semaphore()
    partners = [at(j) for j, _ in near_to] + [at(j) for j, _ in z_to] + [at(j) for j in y_to] + [at(x_to)]
    partners += [at(up), at(down), at(i, 1 - r), at(up, 1 - r), at(down, 1 - r)]
    for partner in partners:
        pl.semaphore_signal(barrier, inc=1, device_id=partner, device_id_type=MESH)

    edge = jnp.zeros((5, 16, 8, 128), F32)
    for n in range(2):
        E[n, :, 4:20, 0:8, :] = edge
        E[n, :, 4:20, 32:40, :] = edge
    for low in (0, 32):
        mid[:, :, low:low + 8, :] = edge
        face_pad[:, :, low:low + 8, :] = jnp.zeros((5, 2, 8, 128), F32)
        fix_pad[:, low:low + 8, :] = jnp.zeros((5, 8, 128), F32)

    source = lax.broadcasted_iota(jnp.int32, (128, 128), 0)
    target = lax.broadcasted_iota(jnp.int32, (128, 128), 1)
    weight = jnp.zeros((128, 128), F32)
    for j in range(1, 5):
        weight = jnp.where(source - target == j, STENCIL[j - 1], jnp.where(target - source == j, -STENCIL[j - 1], weight))
    same_cell = source // 16 == target // 16
    same_frame = source // 8 == target // 8
    inside[...] = jnp.where(same_frame, weight, 0.0)
    across[...] = jnp.where(same_cell & ~same_frame, weight, 0.0)

    lane = lanes()
    cell_of = (lane // 16 + 4) % 8
    upper = lane % 16 >= 8
    row = lax.broadcasted_iota(jnp.int32, (8, 128), 0)

    def spread_cells(get):
        value = jnp.full((8, 128), get(0))
        for a in range(1, 8):
            value = jnp.where(cell_of == a, get(a), value)
        return value

    def weights(t, m):
        up_one, down_one, down_two = t + 1.0, t - 1.0, t - 2.0
        w = (-t * down_one * down_two / 6.0, up_one * down_one * down_two / 2.0,
             -up_one * t * down_two / 2.0, up_one * t * down_one / 6.0)
        value = jnp.zeros((8, 128), F32)
        for p in range(4):
            value = jnp.where(m == p, w[p], value)
        return value

    def pack_rows(n, t, f):
        rows = pl.ds(pl.multiple_of(row0 + 8 * t, 8), 8)
        packed = None
        for a in range(8):
            turned = moved(E[n, f, 8 + a, rows, :], 56 - 16 * ((a + 4) % 8))
            packed = turned if packed is None else jnp.where(cell_of == a, turned, packed)
        return packed

    for copy in loads:
        copy.wait()
    for f in range(5):
        near_a[0][2 + core, f] = pack_rows(0, 0, f)
        ys_b[0][y, f] = pack_rows(0, 1, f)
    stator_t = spread_cells(lambda a: fraction_ref[0, a])
    rotor_t = spread_cells(lambda a: fraction_ref[1, a])
    for n in range(2):
        stator = weights(stator_t, row - spread_cells(lambda a: shift_ref[n, a] + start_ref[0, a] + 3))
        rotor = weights(rotor_t, row - spread_cells(lambda a: start_ref[1, a] - shift_ref[n, a]))
        own_coef[1, n] = jnp.where(upper, stator, rotor)
        near_a[n][2 + core, 5] = jnp.where(upper, rotor, stator)

    pl.semaphore_wait(barrier, len(partners))
    fixed = []

    def send_fixed(src, dst, to):
        no = len(fixed)
        copy = pltpu.make_async_remote_copy(src, dst, fixed_send.at[no], fixed_recv.at[no], device_id=to, device_id_type=MESH)
        copy.start()
        fixed.append(copy)

    half = lane % 64
    ahead = [jnp.where(half + j < 64, STENCIL[j - 1], 0.0) for j in range(1, 5)]
    behind = [jnp.where(half - j >= 0, STENCIL[j - 1], 0.0) for j in range(1, 5)]

    def taps(value, fore, aft):
        total = None
        for j in range(1, 5):
            term = fore[j - 1][0:1] * moved(value, j) - aft[j - 1][0:1] * moved(value, -j)
            total = term if total is None else total + term
        return total

    def product(parts, matrix):
        rows = parts[0].shape[0]
        whole = jnp.dot(jnp.concatenate(parts, axis=0), matrix[...], precision=lax.Precision.HIGHEST, preferred_element_type=F32)
        return [whole[rows * m:rows * m + rows] for m in range(len(parts))]

    def ring(sectors):
        low = lanes(sectors[0].shape[0]) < 64
        return [jnp.where(low, sectors[p], sectors[(p + 1) % 3]) for p in range(3)]

    def by_cells(packs, d):
        if d == 0:
            return packs[:2]
        at_lane = lanes(packs[0].shape[0])
        turned = [moved(v, 16 * d) for v in packs]
        if d > 0:
            return [jnp.where(at_lane < 128 - 16 * d, turned[p], turned[p + 1]) for p in range(2)]
        return [jnp.where(at_lane >= -16 * d, turned[p], turned[(p + 2) % 3]) for p in range(2)]

    def own_cells(packs, d):
        at_lane = lanes(packs[0].shape[0])
        first, last = (moved(v, 16 * d) for v in packs)
        if d >= 0:
            return jnp.where((at_lane >= 64) & (at_lane < 128 - 16 * d), first, last)
        return jnp.where((at_lane < 64) & (at_lane >= -16 * d), last, first)

    def evaluate_rows(ref, c, low):
        dx, dr, da, mine = [], [], [], []
        rows = pl.ds(low, 8)
        for f in range(5):
            here = ref[f, c, rows, :]
            mine.append(here)
            dx.append(taps(here, ahead, behind))
            radial = azimuthal = None
            for j in range(1, 5):
                step = STENCIL[j - 1] * (ref[f, c, pl.ds(low + j, 8), :] - ref[f, c, pl.ds(low - j, 8), :])
                radial = step if radial is None else radial + step
                step = STENCIL[j - 1] * (ref[f, c + j, rows, :] - ref[f, c - j, rows, :])
                azimuthal = step if azimuthal is None else azimuthal + step
            dr.append(radial)
            da.append(azimuthal)
        u = [flow[k, pl.ds(pl.multiple_of(low - 8, 8), 8), :] for k in range(3)]
        push = forcing(dx, dr, da)
        return mine, [-(u[0] * dx[f] + u[1] * dr[f] + u[2] * da[f]) - push[f] for f in range(5)]

    def radial_of(ref, *index):
        total = None
        for j in range(1, 5):
            part = STENCIL[j - 1] * (ref[(*index, slice(8 + j, 32 + j))] - ref[(*index, slice(8 - j, 32 - j))])
            total = part if total is None else total + part
        return total

    def own_rows_of(value):
        return jnp.where(r == 0, value[0:16], value[8:24])

    def widened(f, t, a):
        change = own_fix[f, 0, 8 * t:8 * t + 8, :]
        return jnp.where((lane >= 56) & (lane < 72), moved(change, 16 * ((a + 4) % 8) - 56), 0.0)

    def step(n):
        k = offset_ref[n]
        source_r = (i - k + N) % N
        source_s = (i + k) % N
        low_r = (core - k % 16 + 16) % 16
        low_s = (core + k % 16) % 16
        started = []

        def parts(low):
            far = ((low // 2 + 3) % 8 + 1) // 3 - 1
            near = (low // 2 + 3) % 8 - 3 - 3 * far
            return near, far

        def send(src, dst, to):
            no = len(started)
            copy = pltpu.make_async_remote_copy(src, dst, send_sem.at[n, no], recv_sem.at[n, no], device_id=to, device_id_type=MESH)
            copy.start()
            started.append(copy)
            return copy

        def chosen(slots, from_r, from_s):
            return jnp.where(upper[None], slots[from_r], slots[from_s])

        def along(slots, own, targets):
            mine = slots.at[own]
            return [send(mine, slots.at[place], at(j)) for j, place in targets]

        def arrived(copies):
            for copy in copies:
                copy.wait_recv()

        low = i % 16
        high = i // 16
        high_r = (high - k // 16 - (low + k % 16) // 16 + 16) % 8
        high_s = (high + k // 16 + (k % 16 + 15 - low) // 16) % 8
        (near_r, far_r), (near_s, far_s) = parts(low_r), parts(low_s)
        near_of = (2 * (near_r + 1) + low_r % 2, 2 * (near_s + 1) + low_s % 2)
        ys = [(j, y) for j in y_to]
        xs = [(x_to, x)]

        stage_a = along(near_a[n], 2 + core, near_to)
        stage_b = along(ys_b[n], y, ys)

        if n == 0:
            send_fixed(own_coef.at[1], own_coef.at[0], at(up))
            send_fixed(own_coef.at[1], own_coef.at[2], at(down))
            send_fixed(flow.at[:, pl.ds(8, 8), :], flow.at[:, pl.ds(pl.multiple_of(16 * r, 8), 8), :], at(i, 1 - r))
        else:
            def into_rows(f, carry):
                for t in range(2):
                    rows = pl.ds(pl.multiple_of(row0 + 8 * t, 8), 8)
                    for a in range(8):
                        E[1, f, 8 + a, rows, :] = E[1, f, 8 + a, rows, :] + widened(f, t, a)
                return carry

            lax.fori_loop(0, 5, into_rows, 0)

        own_rows, far_rows = pl.ds(row0, 16), pl.ds(far0, 8)
        halos = []

        def halo_cells(fields):
            part = E.at[n, fields, pl.ds(8, 8), own_rows, :]
            halos.append(send(part, E.at[n, fields, pl.ds(0, 8), own_rows, :], at(up)))
            halos.append(send(part, E.at[n, fields, pl.ds(16, 8), own_rows, :], at(down)))

        def halo_rows(fields):
            halos.append(send(E.at[n, fields, pl.ds(8, 8), pl.ds(16, 8), :], E.at[n, fields, pl.ds(8, 8), far_rows, :], at(i, 1 - r)))

        halo_rows(pl.ds(0, 3))
        halo_cells(pl.ds(0, 2))
        arrived(stage_a)
        far_a[n][1] = chosen(near_a[n], *near_of)
        stage_a = along(far_a[n], 1, z_to)
        arrived(stage_b)
        xs_b[n][x] = chosen(ys_b[n], high_r % NY, high_s % NY)
        stage_b = along(xs_b[n], x, xs)
        halo_cells(pl.ds(2, 2))

        arrived(stage_b)
        near_b[n][2 + core] = chosen(xs_b[n], high_r // NY, high_s // NY)
        stage_b = along(near_b[n], 2 + core, near_to)
        halo_rows(pl.ds(3, 2))
        halos.append(send(E.at[n, :, pl.ds(12, 4), pl.ds(16, 8), :], E.at[n, :, pl.ds(4, 4), far_rows, :], at(up, 1 - r)))
        halos.append(send(E.at[n, :, pl.ds(8, 4), pl.ds(16, 8), :], E.at[n, :, pl.ds(16, 4), far_rows, :], at(down, 1 - r)))
        arrived(stage_a)
        ys_a[n][y] = chosen(far_a[n], far_r + 1, far_s + 1)
        stage_a = along(ys_a[n], y, ys)
        halo_cells(pl.ds(4, 1))

        arrived(stage_b)
        far_b[n][1] = chosen(near_b[n], *near_of)
        stage_b = along(far_b[n], 1, z_to)
        arrived(stage_a)
        xs_a[n][x] = chosen(ys_a[n], (source_r // 16) % NY, (source_s // 16) % NY)
        stage_a = along(xs_a[n], x, xs)

        if n == 0:
            for copy in fixed:
                copy.wait()
            for m in range(3):
                packed = None
                for a in range(8):
                    turned = moved(flow[m], 56 - 16 * a)
                    packed = turned if packed is None else jnp.where(lanes(24) // 16 == a, turned, packed)
                flow_pack[m] = packed
        arrived(stage_a)
        got = chosen(xs_a[n], source_r // 64, source_s // 64)
        facing[n, 1, pl.ds(5 * r, 5)] = got[0:5]
        facing[n, 1, 15] = got[5]
        arrived(stage_b)
        facing[n, 1, pl.ds(5 * r + 5, 5)] = chosen(far_b[n], far_r + 1, far_s + 1)
        rows10, rows5 = pl.ds(5 * r, 10), pl.ds(10 * r, 5)
        stage = []
        for to, place in ((up, 0), (down, 2)):
            stage.append(send(facing.at[n, 1, rows10], facing.at[n, place, rows10], at(to)))
            stage.append(send(facing.at[n, 1, 15], facing.at[n, place, 15], at(to)))
            stage.append(send(facing.at[n, 1, pl.ds(5, 5)], facing.at[n, place, rows5], at(to, 1 - r)))
        stage.append(send(facing.at[n, 1, pl.ds(5, 5)], facing.at[n, 1, rows5], at(i, 1 - r)))

        for copy in halos:
            copy.wait_recv()

        def midpoint(c, low):
            here, slopes = evaluate_rows(E.at[n], c + 4, low)
            for f in range(5):
                mid[f, c, pl.ds(low, 8), :] = here[f] + (0.5 * STEP_SIZE) * slopes[f]

        def first(c, carry):
            midpoint(c, row0)
            midpoint(c, pl.multiple_of(row0 + 8, 8))
            return carry

        def first_far(c, carry):
            midpoint(c + 4, far0_here)
            return carry

        lax.fori_loop(0, 16, first, 0, unroll=2)
        lax.fori_loop(0, 8, first_far, 0, unroll=2)
        def second(c, carry):
            for t in range(2):
                low = pl.multiple_of(row0 + 8 * t, 8)
                _, slopes = evaluate_rows(mid, c + 4, low)
                for f in range(5):
                    E[n + 1, f, c + 8, pl.ds(low, 8), :] = E[n, f, c + 8, pl.ds(low, 8), :] + STEP_SIZE * slopes[f]
            return carry

        lax.fori_loop(0, 8, second, 0, unroll=2)
        if n == 1:
            pltpu.make_async_copy(*result, local_sem.at[0]).start()

        def strip_of(f, carry):
            packs = []
            for p in range(3):
                packed = None
                for a in range(8):
                    turned = moved(E[n, f, (4 + 8 * p + a) % 24, own_rows, :], 56 - 16 * a)
                    packed = turned if packed is None else jnp.where(lanes(16) // 16 == a, turned, packed)
                packs.append(packed)
            for d in range(-4, 4):
                for p, shifted in enumerate(by_cells(packs, d)):
                    own_shifted[f, d + 4, p] = shifted
            if n == 0:
                for t in range(2):
                    next_pack[f, 8 * t:8 * t + 8, :] = pack_rows(1, t, f)
            return carry

        lax.fori_loop(0, 5, strip_of, 0)
        coef_own = ring([own_coef[p, n] for p in range(3)])
        u24 = [flow_pack[m] for m in range(3)]
        u = [flow_pack[m, pl.ds(pl.multiple_of(8 * r, 8), 16), :] for m in range(3)]
        for copy in stage:
            copy.wait_recv()

        coef_face = ring([jnp.where(upper, moved(facing[n, p, 15], -8), moved(facing[n, p, 15], 8)) for p in range(3)])

        all_face, all_ghost_own, all_ghost_face = [], [], []
        for f in range(5):
            F = ring([jnp.concatenate([facing[n, p, 5 * t + f] for t in range(3)], axis=0) for p in range(3)])
            F_own = [own_rows_of(v) for v in F]
            for p in range(2):
                face_pad[f, p, 8:32, :] = F[p]
            ghost_own = [jnp.zeros((24, 128), F32)] * 2
            ghost_face = [jnp.zeros((16, 128), F32)] * 2
            azimuthal = [jnp.zeros((16, 128), F32)] * 2
            for d in range(-4, 5):
                shifted = by_cells(F if d < 4 else F_own, d)
                for p in range(2):
                    if d != 0:
                        weight = STENCIL[d - 1] if d > 0 else -STENCIL[-d - 1]
                        azimuthal[p] = azimuthal[p] + weight * (own_rows_of(shifted[p]) if d < 4 else shifted[p])
                    if d < 4:
                        ghost_own[p] = ghost_own[p] + coef_own[p][d + 4:d + 5, :] * shifted[p]
                        ghost_face[p] = ghost_face[p] + coef_face[p][d + 4:d + 5, :] * own_shifted[f, d + 4, p]
            for p in range(2):
                slope[1, f, p] = own_rows_of(radial_of(face_pad, f, p))
                slope[2, f, p] = azimuthal[p]
            all_face += F_own[:2]
            all_ghost_own += ghost_own
            all_ghost_face += ghost_face
        for m, (a, b) in enumerate(zip(product(all_face, inside), product(all_ghost_face, across))):
            slope[0, m // 2, m % 2] = a + b
        for m, a in enumerate(product(all_ghost_own, across)):
            own_fix[m // 2, m % 2] = a

        for p in range(2):
            dx, dr, da = ([slope[m, f, p] for f in range(5)] for m in range(3))
            push = forcing(dx, dr, da)
            for f in range(5):
                change = -(u[0] * dx[f] + u[1] * dr[f] + u[2] * da[f]) - push[f]
                face_mid[f, p] = face_pad[f, p, own_rows, :] + (0.5 * STEP_SIZE) * change
            cut = [own_fix[f, p] for f in range(5)]
            push = [cut[1], cut[4], 0.0, 0.0, cut[1]]
            for f in range(5):
                own_fix[f, p] = (-0.5 * STEP_SIZE) * (u24[0] * cut[f] + push[f])

        all_fix, all_ghost = [], []
        for f in range(5):
            face = [face_mid[f, p] for p in range(2)]
            fix = [own_rows_of(own_fix[f, p]) for p in range(2)]
            fix_pad[f, 8:32, :] = own_cells([own_fix[f, p] for p in range(2)], 0)
            ghosts = jnp.zeros((16, 128), F32)
            azimuthal = jnp.zeros((16, 128), F32)
            for d in range(-4, 5):
                if d < 4:
                    ghosts = ghosts + own_coef[1, n, d + 4:d + 5, :] * own_cells(face, d)
                if d != 0:
                    weight = STENCIL[d - 1] if d > 0 else -STENCIL[-d - 1]
                    azimuthal = azimuthal + weight * own_cells(fix, d)
            all_fix.append(own_cells(fix, 0))
            all_ghost.append(ghosts)
            slope[1, f, 0] = own_rows_of(radial_of(fix_pad, f))
            slope[2, f, 0] = azimuthal
        dx = [a + b for a, b in zip(product(all_fix, inside), product(all_ghost, across))]
        dr, da = ([slope[m, f, 0] for f in range(5)] for m in range(1, 3))
        push = forcing(dx, dr, da)
        for f in range(5):
            change = -STEP_SIZE * (u[0] * dx[f] + u[1] * dr[f] + u[2] * da[f] + push[f])
            own_fix[f, 0, 0:16, :] = change
            if n == 0:
                after = next_pack[f] + change
                near_a[1][2 + core, f] = after[0:8]
                ys_b[1][y, f] = after[8:16]
        return started

    result = (E.at[2, :, pl.ds(8, 8), pl.ds(row0, 16), :], out_hbm)
    started = step(0)
    started += step(1)

    def into_fix(f, carry):
        for t in range(2):
            for a in range(8):
                wide_fix[f, a, 8 * t:8 * t + 8, :] = widened(f, t, a)
        return carry

    lax.fori_loop(0, 5, into_fix, 0)
    store_fix = pltpu.make_async_copy(wide_fix, fix_hbm, local_sem.at[1])
    store_fix.start()
    for copy in started:
        copy.wait_send()
    pltpu.make_async_copy(*result, local_sem.at[0]).wait()
    store_fix.wait()


def shards(acoustic_state, mean_flow, sector_offset, cell_shift, stencil_start, interface_fraction):
    anywhere = pl.BlockSpec(memory_space=pl.ANY)
    vmem = lambda *shape: pltpu.VMEM(shape, F32)
    smem = lambda value: pltpu.SMEM(value.shape, value.dtype)
    without, ghosts = pl.pallas_call(
        kernel,
        out_shape=[jax.ShapeDtypeStruct(acoustic_state.shape, F32)] * 2,
        in_specs=[anywhere] * 6,
        out_specs=[anywhere] * 2,
        scratch_shapes=[
            smem(sector_offset),
            smem(cell_shift),
            smem(stencil_start),
            smem(interface_fraction),
            vmem(3, 5, 24, 40, 128),
            vmem(5, 16, 40, 128),
            *[vmem(count, tiles, 8, 128) for count in (6, 3, NY, NX) for tiles in (6, 5) for _ in range(2)],
            vmem(2, 3, 16, 8, 128),
            vmem(3, 2, 8, 128),
            vmem(3, 24, 128),
            vmem(3, 24, 128),
            vmem(5, 2, 40, 128),
            vmem(3, 5, 2, 16, 128),
            vmem(5, 2, 16, 128),
            vmem(5, 2, 24, 128),
            vmem(5, 16, 128),
            vmem(5, 40, 128),
            vmem(5, 8, 16, 128),
            vmem(128, 128),
            vmem(128, 128),
            vmem(5, 8, 2, 16, 128),
            pltpu.SemaphoreType.DMA((2, 40)),
            pltpu.SemaphoreType.DMA((2, 40)),
            pltpu.SemaphoreType.DMA((3,)),
            pltpu.SemaphoreType.DMA((3,)),
            pltpu.SemaphoreType.DMA((6,)),
        ],
        compiler_params=pltpu.CompilerParams(collective_id=0, has_side_effects=True, vmem_limit_bytes=67043328),
        name="acoustic_steps",
    )(sector_offset, cell_shift, stencil_start, interface_fraction, mean_flow, acoustic_state)
    return without + ghosts


def solution(mesh):
    return jax.shard_map(
        shards,
        mesh=mesh,
        in_specs=(
            P(None, "azim", "rad", None),
            P(None, "rad", None),
            P(),
            P(None, "azim"),
            P(None, "azim"),
            P(None, "azim"),
        ),
        out_specs=P(None, "azim", "rad", None),
        check_vma=False,
    )
```
